32 devices in a mesh: graphs: 2 (over y), rows: 4 (over z), cols: 2 (over x), sub: 2 (over core).
Axes of the slice: x: 2, y: 2, z: 4, core: 2. Of those that a mesh axis runs over, the one named last changes fastest.
Arguments:
- current_block: float32 [16, 65536], P(None, ('graphs', 'rows', 'cols', 'sub')), parts along dimension 1, may hold values from -1200 to 1200, as said below
- previous_block: float32 [16, 65536], P(None, ('graphs', 'rows', 'cols', 'sub')), parts along dimension 1, may hold values from -1200 to 1200, as said below
- adjacency_tiles: float32 [1536, 128, 128], P(('graphs', 'rows', 'cols', 'sub')), parts along dimension 0, may hold values from -0.3125 to 0.3125
- tile_rows: int32 [1536], P(('graphs', 'rows', 'cols', 'sub')), parts along dimension 0, may hold values from 0 to 255, as said below
- tile_cols: int32 [1536], P(('graphs', 'rows', 'cols', 'sub')), parts along dimension 0, may hold values from 0 to 255, as said below
- tile_count: int32 [32], P(('graphs', 'rows', 'cols', 'sub')), parts along dimension 0, may hold values from 18 to 48, as said below
- locked: int32 [2], P('graphs'), parts along dimension 0, may hold values from 0 to 7
Outputs:
- w_basis: float32 [16, 65536], P(None, ('graphs', 'rows', 'cols', 'sub')), parts along dimension 1
- w_image: float32 [16, 65536], P(None, ('graphs', 'rows', 'cols', 'sub')), parts along dimension 1
- ritz_matrix: float32 [96, 48], P('graphs'), parts along dimension 0
The draws below stay inside these ranges and needn't reach their ends.
There are 2 independent parts, one for each index of `graphs`. The reference program is written for one: setup_inputs(seed, part) draws one part's arguments, and reference() takes and returns one part's arrays. A program takes and returns all parts, laid end to end along the dimension named above; each array names one. Nothing has to cross between parts.
Inputs may be any that keep to these rules, and one draw needn't show every extreme that they name: `current_block`: entries of order one to some hundreds. `previous_block`: entries of order one to some hundreds. Slots d * 48 to (d + 1) * 48 - 1 belong to device d and name its own tile rows d * 16 to (d + 1) * 16 - 1. The first 16 slots of a device name its tile rows in order, with tile_cols equal to tile_rows. Slots past the device's count name tile row d * 16 and carry no weight. `tile_cols`: A slot of device d names a tile column from d * 16 - 8 to (d + 1) * 16 + 7. Slot 16 of a device names a tile of the block before it and slot 17 one of the block after it, where such a block exists. A pair of tile row and tile column may stand in several slots; their tiles add. `tile_count`: in every draw some device has all 48 slots live.
All inputs are finite; a program needn't handle non-finite values.
Results may differ from the reference program's by a relative error of at most 0.000094.
Values sent between devices are 32-bit elements; how exact they have to be, the bound alone decides.
A program may use at most 64 MiB of HBM per device.

```python
import jax
import jax.numpy as jnp
from jax import lax

K = 16
TILE_VERTICES = 128
DEVICE_SLOTS = 3
DEVS = 16
DEVICE_TILE_ROWS = 16
REACH = 8
MAXT_DEV = 48
NV = 32768
NT = 256
GRAPH_SLOTS = 768


def tile_arrangement(key):
    keys = jax.random.split(jax.random.fold_in(key, 11), 6)
    devices = jnp.arange(DEVS, dtype=jnp.int32)
    slot_indices = jnp.arange(MAXT_DEV, dtype=jnp.int32)[None, :]
    extra = jax.random.randint(keys[0], (DEVS,), 2, MAXT_DEV - DEVICE_TILE_ROWS + 1)
    fullest = jax.random.randint(keys[1], (), 0, DEVS)
    extra = jnp.where(devices == fullest, MAXT_DEV - DEVICE_TILE_ROWS, extra)
    counts = (DEVICE_TILE_ROWS + extra).astype(jnp.int32)
    row_offset = jax.random.randint(keys[2], (DEVS, MAXT_DEV), 0, DEVICE_TILE_ROWS)
    col_offset = jax.random.randint(keys[3], (DEVS, MAXT_DEV), -REACH, DEVICE_TILE_ROWS + REACH)
    left_offset = jax.random.randint(keys[4], (DEVS, MAXT_DEV), -REACH, 0)
    right_offset = DEVICE_TILE_ROWS + jax.random.randint(keys[5], (DEVS, MAXT_DEV), 0, REACH)
    col_offset = jnp.where(slot_indices == DEVICE_TILE_ROWS, left_offset, col_offset)
    col_offset = jnp.where(slot_indices == DEVICE_TILE_ROWS + 1, right_offset, col_offset)
    diagonal = slot_indices < DEVICE_TILE_ROWS
    row_offset = jnp.where(diagonal, slot_indices, row_offset)
    col_offset = jnp.where(diagonal, slot_indices, col_offset)
    padded = slot_indices >= counts[:, None]
    row_offset = jnp.where(padded, 0, row_offset)
    col_offset = jnp.where(padded, 0, col_offset)
    rows_out = devices[:, None] * DEVICE_TILE_ROWS + row_offset
    cols_out = devices[:, None] * DEVICE_TILE_ROWS + col_offset
    cols_out = jnp.where(cols_out < 0, cols_out + REACH, cols_out)
    cols_out = jnp.where(cols_out >= NT, cols_out - REACH, cols_out)
    return (rows_out.reshape(-1).astype(jnp.int32), cols_out.reshape(-1).astype(jnp.int32), counts)


def draw_tile_rows(key, part):
    return tile_arrangement(key)[0]


def draw_tile_cols(key, part):
    return tile_arrangement(key)[1]


def draw_tile_count(key, part):
    return tile_arrangement(key)[2]


def draw_locked(key, part):
    base = jax.random.randint(jax.random.fold_in(key, 53), (1,), 0, 7)
    return jnp.where(part % 2 == 1, 7, base).astype(jnp.int32)


def vector_draw(key):
    keys = jax.random.split(key, 4)
    where_along = jnp.arange(NV, dtype=jnp.float32) / NV
    rising = jnp.sqrt(1.0 + 2.0 * where_along)
    base = jax.random.truncated_normal(keys[0], -5.0, 5.0, (K, NV), jnp.float32)
    rough = 10.0 ** jax.random.uniform(keys[2], (NV,), jnp.float32)
    column_scale = 10.0 ** jax.random.uniform(keys[3], (K,), jnp.float32)
    return base * (rough * rising)[None, :] * column_scale[:, None]


def draw_current_block(key, part):
    return vector_draw(jax.random.fold_in(key, 21))


def draw_previous_block(key, part):
    return vector_draw(jax.random.fold_in(key, 37))


def shard_levels(rng, dims, cuts, smallest, high):
    loudness = 1.0
    for dim, blocks in cuts:
        draws = jax.random.uniform(jax.random.fold_in(jax.random.fold_in(rng, 6), dim), (blocks,), jnp.float32, smallest / len(cuts), high / len(cuts))
        loudness = loudness * jnp.repeat(jnp.exp(draws), dims[dim] // blocks).reshape((-1,) + (1,) * (len(dims) - 1 - dim))
    return loudness


def normal_values(rng, dims, spread, most, shards=(), kind=jnp.bfloat16):
    drawn = spread * jax.random.normal(rng, dims, jnp.float32)
    if shards:
        drawn = drawn * shard_levels(rng, dims, shards, -0.22, 0.18)
    return jnp.clip(drawn, -most, most).astype(kind)


def setup_inputs(seed: int = 0, part: int = 0) -> dict:
    splits = jax.random.split(jax.random.key(seed), 8)
    own_keys = jax.random.split(jax.random.fold_in(splits[7], part), 8)
    return {
        "current_block": draw_current_block(jax.random.fold_in(jax.random.fold_in(splits[7], part), 71), part),
        "previous_block": draw_previous_block(jax.random.fold_in(jax.random.fold_in(splits[7], part), 71), part),
        "adjacency_tiles": normal_values(own_keys[2], (GRAPH_SLOTS, TILE_VERTICES, TILE_VERTICES), (DEVICE_SLOTS * TILE_VERTICES) ** -0.5, 0.3125, ((0, 16),), jnp.float32),
        "tile_rows": draw_tile_rows(jax.random.fold_in(jax.random.fold_in(splits[7], part), 71), part),
        "tile_cols": draw_tile_cols(jax.random.fold_in(jax.random.fold_in(splits[7], part), 71), part),
        "tile_count": draw_tile_count(jax.random.fold_in(jax.random.fold_in(splits[7], part), 71), part),
        "locked": draw_locked(jax.random.fold_in(jax.random.fold_in(splits[7], part), 71), part),
    }


def apply_operator(vectors, adjacency_tiles, tile_rows, tile_cols, live_mask):
    channels = vectors.shape[0]
    column_blocks = vectors.reshape(channels, NT, TILE_VERTICES)
    gathered = jnp.take(column_blocks, tile_cols, axis=1)
    products = jnp.einsum('cta,tab->tcb', gathered, adjacency_tiles, precision=lax.Precision.HIGHEST)
    products = products * live_mask[:, None, None]
    summed = jax.ops.segment_sum(products, tile_rows, num_segments=NT)
    return vectors - jnp.transpose(summed, (1, 0, 2)).reshape(channels, NV)

def inner_products(left, right):
    return jnp.dot(left, right.T, precision=lax.Precision.HIGHEST)

def rayleigh_ritz(gram_b, gram_a):
    factor_b = jnp.linalg.cholesky(gram_b)
    symmetric = 0.5 * (gram_a + gram_a.T)
    halfway = lax.linalg.triangular_solve(factor_b, symmetric, left_side=True, lower=True)
    return lax.linalg.triangular_solve(factor_b, halfway.T, left_side=True, lower=True)

def reference(current_block, previous_block, adjacency_tiles, tile_rows, tile_cols, tile_count, locked):
    slot_indices = jnp.arange(GRAPH_SLOTS, dtype=jnp.int32)
    owners = slot_indices // MAXT_DEV
    live_mask = (slot_indices % MAXT_DEV < tile_count[owners]).astype(jnp.float32)
    stacked = jnp.concatenate([current_block, previous_block], axis=0)
    images = apply_operator(stacked, adjacency_tiles, tile_rows, tile_cols, live_mask)
    x_image = images[:K]
    p_image = images[K:]
    quotient = jnp.sum(current_block * x_image, axis=1) / (jnp.sum(current_block * current_block, axis=1) + 1e-06)
    frozen_rows = jnp.arange(K, dtype=jnp.int32) < locked[0]
    residual = jnp.where(frozen_rows[:, None], 0.0, x_image - quotient[:, None] * current_block)
    gram_w = inner_products(residual, residual) / NV + jnp.diag(frozen_rows.astype(jnp.float32))
    factor = jnp.linalg.cholesky(gram_w)
    w_basis = lax.linalg.triangular_solve(factor, residual, left_side=True, lower=True)
    w_image = apply_operator(w_basis, adjacency_tiles, tile_rows, tile_cols, live_mask)
    search = jnp.concatenate([current_block, w_basis, previous_block], axis=0)
    search_image = jnp.concatenate([x_image, w_image, p_image], axis=0)
    zero_rows = jnp.zeros((K,), jnp.float32)
    pad_diag = jnp.concatenate([zero_rows, frozen_rows.astype(jnp.float32), zero_rows])
    gram_b = inner_products(search, search) / NV + jnp.diag(pad_diag)
    gram_a = inner_products(search, search_image) / NV
    ritz_matrix = rayleigh_ritz(gram_b, gram_a)
    return (w_basis, w_image, ritz_matrix)
```

```python
import functools

import jax
import jax.numpy as jnp
from jax import lax
from jax.experimental import pallas as pl
from jax.experimental.pallas import tpu as pltpu
from jax.sharding import PartitionSpec as P

MESH = pl.DeviceIdType.MESH
F32 = jnp.float32
BF16 = jnp.bfloat16
HIGHEST = lax.Precision.HIGHEST
NT_DIMS = (((1,), (1,)), ((), ()))
EDGE = 8
VMEM_ALL = 67043328
VMEM_ROOM = 10600 * 1024


def split(values):
    high = values.astype(BF16)
    return high, (values - high.astype(F32)).astype(BF16)


def iota(shape, dim):
    return lax.broadcasted_iota(jnp.int32, shape, dim)


def tree_sum(terms):
    while len(terms) > 1:
        terms = [a + b for a, b in zip(terms[::2], terms[1::2])] + terms[len(terms) & ~1 :]
    return terms[0]


def panel(matrix, k, shift, count):
    rows = [matrix[k + i : k + i + 1, :] for i in range(count)]
    columns = [
        jnp.broadcast_to(matrix[:, shift + k + i : shift + k + i + 1], matrix.shape)
        for i in range(count)
    ]
    block = {
        (i, j): jnp.broadcast_to(rows[i][:, shift + k + j : shift + k + j + 1], (1, 128))
        for i in range(count)
        for j in range(i, count)
    }
    done = []
    for m in range(count):
        inverse = 1.0 / block[m, m]
        done.append(rows[m] * lax.rsqrt(block[m, m]))
        factors = {j: block[m, j] * inverse for j in range(m + 1, count)}
        for i in range(m + 1, count):
            for j in range(i, count):
                block[i, j] = block[i, j] - factors[i] * block[m, j]
            rows[i] = rows[i] - factors[i] * rows[m]
            columns[i] = columns[i] - factors[i] * columns[m]
        matrix = matrix - columns[m] * (rows[m] * inverse)
    return matrix, done


def iterate_kernel(
    sizes, vertex_total,
    cols_in, rows_in, count_in, locked_in, x_hbm, p_hbm, tiles_hbm,
    w_ref, aw_ref, ritz_ref,
    cols_ref, rows_ref, count_ref, locked_ref, index_ref, before_ref, last_ref,
    raw, halves, xh, ph, yh, q_buf, z_buf, seg, mine, every, upper,
    int_sem, block_sem, tile_sem, halo_send, halo_recv, all_send, all_recv,
):
    row_count, col_count, sub_count = sizes
    near_count = col_count * sub_count
    total = row_count * near_count
    vectors, here = w_ref.shape
    slots, tile, _ = raw.shape
    row_tiles = here // tile
    reach = row_tiles // 2
    spare = slots - row_tiles
    chunk = row_tiles
    chunks = slots // chunk
    width = 3 * vectors

    row_at = lax.axis_index("rows")
    col_at = lax.axis_index("cols")
    sub_at = lax.axis_index("sub")
    position = row_at * near_count + col_at * sub_count + sub_at

    def place(spot):
        return {
            "rows": lax.div(spot, near_count),
            "cols": lax.div(lax.rem(spot, near_count), sub_count),
            "sub": lax.rem(spot, sub_count),
        }

    rows_from = [lax.rem(row_at + k, row_count) for k in range(row_count)]
    cols_from = [lax.rem(col_at + k, col_count) for k in range(col_count)]
    subs_from = [lax.rem(sub_at + k, sub_count) for k in range(sub_count)]

    def each_peer(act):
        if total <= 32:
            for k in range(1, total):
                act(
                    {
                        "rows": rows_from[k // near_count],
                        "cols": cols_from[k % near_count // sub_count],
                        "sub": subs_from[k % sub_count],
                    }
                )
        else:

            def step(k, carry):
                act(place(lax.rem(position + k, total)))
                return carry

            lax.fori_loop(1, total, step, 0)

    barrier = pltpu.get_barrier_semaphore()
    each_peer(
        lambda device: pl.semaphore_signal(barrier, inc=1, device_id=device, device_id_type=MESH)
    )

    own = pl.ds(reach, row_tiles)

    def block_start(source, target, sem):
        for t in range(row_tiles):
            pltpu.make_async_copy(
                source.at[:, pl.ds(t * tile, tile)], target.at[reach + t], sem
            ).start()

    def block_wait(target, sem):
        pltpu.make_async_copy(target.at[own], target.at[own], sem).wait()

    block_start(x_hbm, xh, block_sem.at[0])
    int_copies = [
        pltpu.make_async_copy(source, target, int_sem.at[i])
        for i, (source, target) in enumerate(
            (
                (cols_in, cols_ref),
                (rows_in, rows_ref),
                (count_in, count_ref),
                (locked_in, locked_ref),
            )
        )
    ]
    for copy in int_copies:
        copy.start()
    tile_copies = []
    for c in range(chunks):
        part = pl.ds(c * chunk, chunk)
        tile_copies.append(pltpu.make_async_copy(tiles_hbm.at[part], raw.at[part], tile_sem.at[c]))
    tile_copies[0].start()
    block_start(p_hbm, ph, block_sem.at[1])
    for copy in tile_copies[1:]:
        copy.start()

    has_left = position > 0
    has_right = position < total - 1
    left_device = place(lax.max(position - 1, 0))
    right_device = place(lax.min(position + 1, total - 1))

    def halo_copies(buffer, which):
        left = pltpu.make_async_remote_copy(
            src_ref=buffer.at[pl.ds(reach, reach)],
            dst_ref=buffer.at[pl.ds(reach + row_tiles, reach)],
            send_sem=halo_send.at[which, 0],
            recv_sem=halo_recv.at[which, 0],
            device_id=left_device,
            device_id_type=MESH,
        )
        right = pltpu.make_async_remote_copy(
            src_ref=buffer.at[pl.ds(row_tiles, reach)],
            dst_ref=buffer.at[pl.ds(0, reach)],
            send_sem=halo_send.at[which, 1],
            recv_sem=halo_recv.at[which, 1],
            device_id=right_device,
            device_id_type=MESH,
        )
        return left, right

    def halo_do(first_when, first, second_when, second):
        @pl.when(first_when)
        def _():
            first()

        @pl.when(second_when)
        def _():
            second()

    def halo_start(copies):
        halo_do(has_left, copies[0].start, has_right, copies[1].start)

    def halo_arrived(copies):
        halo_do(has_right, copies[0].wait_recv, has_left, copies[1].wait_recv)

    def halo_sent(copies):
        halo_do(has_left, copies[0].wait_send, has_right, copies[1].wait_send)

    x_halo = halo_copies(xh, 0)
    p_halo = halo_copies(ph, 1)
    y_halo = halo_copies(yh, 2)

    block_wait(xh, block_sem.at[0])
    pl.semaphore_wait(barrier, total - 1)
    halo_start(x_halo)
    block_wait(ph, block_sem.at[1])
    halo_start(p_halo)

    def product(block, slot):
        high, low = split(block)
        lhs = jnp.concatenate(
            [jnp.concatenate([high, high], axis=1), jnp.concatenate([low, low], axis=1)], axis=0
        )
        out = jnp.dot(lhs, halves[slot], preferred_element_type=F32)
        return out[:vectors] + out[vectors:]

    def split_tiles(c):
        tile_copies[c].wait()

        def step(i, carry):
            for j in range(2):
                t = c * chunk + 2 * i + j
                high, low = split(raw[t])
                halves[t, 0:tile, :] = high
                halves[t, tile : 2 * tile, :] = low
            return carry

        lax.fori_loop(0, chunk // 2, step, 0)

    def diagonal(source, target, target_base):
        def step(g, carry):
            for i in range(8):
                r = g * 8 + i
                target[target_base + r] = product(source[reach + r], r)
            return carry

        lax.fori_loop(0, row_tiles // 8, step, 0)

    def tables():
        for copy in int_copies:
            copy.wait()
        live = count_ref[0]
        base_col = position * row_tiles - reach
        base_row = position * row_tiles
        at = []
        for t in range(spare):
            index_ref[t] = jnp.clip(cols_ref[row_tiles + t] - base_col, 0, 2 * row_tiles - 1)
            row = jnp.where(row_tiles + t < live, rows_ref[row_tiles + t] - base_row, -1)
            link = jnp.int32(0)
            for s in range(t):
                link = jnp.where(at[s] == row, s + 1, link)
            before_ref[t] = link
            at.append(row)
        for r in range(row_tiles):
            link = jnp.int32(0)
            for s in range(spare):
                link = jnp.where(at[s] == r, s + 1, link)
            last_ref[r] = link

    def scattered(padded, target, target_base):
        for t in range(spare):
            out = product(padded[index_ref[t]], row_tiles + t)
            seg[t + 1] = out + seg[before_ref[t]]
        for r in range(row_tiles):
            target[target_base + r] = target[target_base + r] + seg[last_ref[r]]

    def parts(buffer, start):
        pieces = [split(buffer[start + t]) for t in range(row_tiles)]
        return [jnp.concatenate([piece[half] for piece in pieces], axis=1) for half in range(2)]

    def inner(left, right):
        lhs = jnp.concatenate([v[0] for v in left] + [v[1] for v in left], axis=0)
        rhs = jnp.concatenate([v[0] for v in right] + [v[1] for v in right], axis=0)
        out = lax.dot_general(lhs, rhs, NT_DIMS, preferred_element_type=F32)
        count = len(left) * vectors
        return out[:count] + out[count:]

    edge_lane = iota((EDGE, 128), 1)

    def pack(values, lanes):
        rows = values.shape[0]
        padded = jnp.concatenate([values, jnp.zeros((rows, 128 - 2 * lanes), F32)], axis=1)
        pieces = []
        for k in range(rows // EDGE):
            piece = padded[k * EDGE : (k + 1) * EDGE]
            first = piece if k == 0 else pltpu.roll(piece, k * lanes, 1)
            second = pltpu.roll(piece, (k * lanes - lanes) % 128, 1)
            here_lane = (edge_lane >= k * lanes) & (edge_lane < (k + 1) * lanes)
            pieces.append(jnp.where(here_lane, first + second, 0.0))
        return tree_sum(pieces)

    def unpack(values, rows, lanes):
        pieces = [
            values if k == 0 else pltpu.roll(values, 128 - k * lanes, 1) for k in range(rows // EDGE)
        ]
        return jnp.concatenate(pieces, axis=0)

    def exchange(which, values):
        mine[which] = values
        each_peer(
            lambda device: pltpu.make_async_remote_copy(
                src_ref=mine.at[which],
                dst_ref=every.at[which, position],
                send_sem=all_send.at[which],
                recv_sem=all_recv.at[which],
                device_id=device,
                device_id_type=MESH,
            ).start()
        )
        every[which, position] = values

    others = pl.ds(0, total - 1)

    def all_wait(which, sem):
        pltpu.make_async_copy(
            every.at[which, others], every.at[which, others], sem.at[which]
        ).wait()

    def collect(which):
        all_wait(which, all_recv)
        if total <= 32:
            return tree_sum([every[which, k] for k in range(total)])
        return lax.fori_loop(
            1, total, lambda k, out: out + every[which, k], every[which, 0]
        )

    tables()
    seg[0] = jnp.zeros((vectors, tile), F32)
    for c in range(chunks):
        split_tiles(c)
        if c == row_tiles // chunk - 1:
            diagonal(xh, yh, reach)
    diagonal(ph, q_buf, 0)
    x_parts, p_parts = parts(xh, reach), parts(ph, reach)
    exchange(0, pack(inner((x_parts, p_parts), (x_parts, p_parts)), 2 * vectors))

    halo_arrived(x_halo)
    scattered(xh, yh, reach)
    halo_start(y_halo)
    y_parts = parts(yh, reach)
    basis = (x_parts, y_parts, p_parts)
    exchange(1, pack(inner(basis, (y_parts,)), vectors))

    halo_arrived(p_halo)
    scattered(ph, q_buf, 0)
    exchange(2, pack(inner(basis, (parts(q_buf, 0),)), vectors))
    diagonal(yh, z_buf, 0)
    halo_arrived(y_halo)
    scattered(yh, z_buf, 0)
    exchange(3, pack(inner(basis, (parts(z_buf, 0),)), vectors))

    scale = 1.0 / vertex_total
    locked = locked_ref[0]
    by_xp = unpack(collect(0), 2 * vectors, 2 * vectors)
    by_y = unpack(collect(1), width, vectors)
    lane_w = iota((vectors, 128), 1)
    line_w = iota((vectors, 128), 0)
    middle_w = (lane_w >= vectors) & (lane_w < 2 * vectors)
    shifted_y = pltpu.roll(by_y, vectors, 1)
    shifted_xp = pltpu.roll(by_xp, vectors, 1)
    on_first = lane_w == line_w
    on_second = lane_w == line_w + vectors
    free_down = iota((vectors, 1), 0) >= locked
    free_along = (iota((1, 128), 1) >= vectors + locked) & (iota((1, 128), 1) < 2 * vectors)

    def diagonal_of(mask, values, axis):
        return jnp.sum(jnp.where(mask, values, 0.0), axis=axis, keepdims=True)

    def ratio(mask, over, under, axis):
        return (diagonal_of(mask, over, axis) + 1e-06) / (diagonal_of(mask, under, axis) + 1e-06)

    down = jnp.where(free_down, ratio(on_first, by_y[:vectors], by_xp[:vectors], 1), 0.0)
    along = jnp.where(
        free_along, ratio(on_second, shifted_y[:vectors], shifted_xp[:vectors], 0), 0.0
    )

    lane = iota((width, 128), 1)
    line = iota((width, 128), 0)
    is_first = lane < vectors
    is_second = (lane >= vectors) & (lane < 2 * vectors)
    is_third = (lane >= 2 * vectors) & (lane < width)
    square = jnp.concatenate(
        [jnp.where(lane < vectors, by_y, 0.0), jnp.zeros((128 - width, 128), F32)], axis=0
    )
    y_rows = jnp.transpose(square)[:vectors]
    zero_w = jnp.zeros((vectors, 128), F32)
    over_x = jnp.concatenate([by_xp[:vectors], y_rows, by_xp[vectors:]], axis=0)
    over_x_next = jnp.concatenate(
        [shifted_xp[:vectors], pltpu.roll(y_rows, vectors, 1), shifted_xp[vectors:]], axis=0
    )
    over_p = jnp.concatenate([shifted_xp[:vectors], y_rows, shifted_xp[vectors:]], axis=0)
    gate = jnp.where(free_along, 1.0, 0.0)

    def residual_rows(values):
        first, second, third = [values[i * vectors : (i + 1) * vectors] for i in range(3)]
        return jnp.concatenate(
            [first, jnp.where(free_down, down * first - second, 0.0), third], axis=0
        )

    def three(first, second, third):
        return jnp.where(
            is_first, first, jnp.where(is_second, second, jnp.where(is_third, third, 0.0))
        )

    gram = residual_rows(
        three(over_x, over_x_next * along - shifted_y * gate, over_p)
    )
    gram = gram * scale

    rest = gram[vectors : 2 * vectors]
    frozen = on_second & (line_w < locked)
    small = jnp.where(middle_w, rest + jnp.where(frozen, 1.0, 0.0), 0.0)
    small = small + jnp.where(lane_w == line_w + 2 * vectors, 1.0, 0.0)
    padded = (line == lane) & (line >= vectors) & (line < vectors + locked)
    big = gram + jnp.where(padded | (lane == line + width), 1.0, 0.0)

    step = 4
    small_rows = []
    for k in range(0, vectors, step):
        small, done = panel(small, k, vectors, step)
        small_rows += done
    inverse_w = jnp.concatenate(small_rows, axis=0)[:, 2 * vectors : 3 * vectors]

    def outputs():
        high, low = split(inverse_w)
        lhs = jnp.concatenate(
            [jnp.concatenate([high, high], axis=1), jnp.concatenate([low, low], axis=1)], axis=0
        )

        def turn(values):
            rhs = jnp.concatenate(split(values), axis=0)
            out = jnp.dot(lhs, rhs, preferred_element_type=F32)
            return out[:vectors] + out[vectors:]

        for t in range(row_tiles):
            lanes = slice(t * tile, (t + 1) * tile)
            image = yh[reach + t]
            residual = jnp.where(free_down, down * xh[reach + t] - image, 0.0)
            carried = jnp.where(free_down, down * image - z_buf[t], 0.0)
            w_ref[:, lanes] = turn(residual)
            aw_ref[:, lanes] = turn(residual - carried)

    for k in range(0, width, step):
        if k == 2 * vectors:
            outputs()
        big, done = panel(big, k, 0, step)
        for i in range(step):
            upper[k + i : k + i + 1, :] = done[i]
    inverse = upper[:, width : 2 * width]

    by_q = unpack(collect(2), width, vectors)
    early = residual_rows(three(by_y, shifted_y * along, pltpu.roll(by_q, 2 * vectors, 1)))
    by_z = unpack(collect(3), width, vectors)
    late = residual_rows(jnp.where(is_second, pltpu.roll(by_z, vectors, 1) * gate, 0.0))
    image = (gram - scale * (early - late))[:, :width]
    half = jnp.dot(inverse, image, precision=HIGHEST, preferred_element_type=F32)
    first = lax.dot_general(half, inverse, NT_DIMS, precision=HIGHEST, preferred_element_type=F32)
    second = lax.dot_general(inverse, half, NT_DIMS, precision=HIGHEST, preferred_element_type=F32)
    ritz_ref[...] = 0.5 * (first + second)

    halo_sent(x_halo)
    halo_sent(p_halo)
    halo_sent(y_halo)
    for which in range(4):
        all_wait(which, all_send)


def store_kernel(w_ref, aw_ref, ritz_ref, w_hbm, aw_hbm, ritz_hbm, sem):
    copies = [
        pltpu.make_async_copy(source, target, sem.at[i])
        for i, (source, target) in enumerate(
            ((w_ref, w_hbm), (aw_ref, aw_hbm), (ritz_ref, ritz_hbm))
        )
    ]
    for copy in copies:
        copy.start()
    for copy in copies:
        copy.wait()


def body(sizes, current_block, previous_block, adjacency_tiles, tile_rows, tile_cols, tile_count, locked):
    vectors, here = current_block.shape
    slots, tile, _ = adjacency_tiles.shape
    row_tiles = here // tile
    row_count, col_count, sub_count = sizes
    total = row_count * col_count * sub_count
    width = 3 * vectors
    spare = slots - row_tiles
    vmem = pl.BlockSpec(memory_space=pltpu.VMEM)
    anywhere = pl.BlockSpec(memory_space=pl.ANY)
    dma = pltpu.SemaphoreType.DMA
    grid = (2 * row_tiles, vectors, tile)
    own = (row_tiles, vectors, tile)
    shapes = (
        jax.ShapeDtypeStruct((vectors, here), F32),
        jax.ShapeDtypeStruct((vectors, here), F32),
        jax.ShapeDtypeStruct((width, width), F32),
    )
    results = pl.pallas_call(
        functools.partial(iterate_kernel, sizes, here * total),
        out_shape=shapes,
        in_specs=[anywhere] * 7,
        out_specs=(vmem, vmem, vmem),
        scratch_shapes=[
            pltpu.SMEM((slots,), jnp.int32),
            pltpu.SMEM((slots,), jnp.int32),
            pltpu.SMEM((1,), jnp.int32),
            pltpu.SMEM((1,), jnp.int32),
            pltpu.SMEM((spare,), jnp.int32),
            pltpu.SMEM((spare,), jnp.int32),
            pltpu.SMEM((row_tiles,), jnp.int32),
            pltpu.VMEM((slots, tile, tile), F32),
            pltpu.VMEM((slots, 2 * tile, tile), BF16),
            pltpu.VMEM(grid, F32),
            pltpu.VMEM(grid, F32),
            pltpu.VMEM(grid, F32),
            pltpu.VMEM(own, F32),
            pltpu.VMEM(own, F32),
            pltpu.VMEM((spare + 1, vectors, tile), F32),
            pltpu.VMEM((4, EDGE, 128), F32),
            pltpu.VMEM((4, total, EDGE, 128), F32),
            pltpu.VMEM((width, 128), F32),
            dma((4,)),
            dma((2,)),
            dma((slots // row_tiles,)),
            dma((3, 2)),
            dma((3, 2)),
            dma((4,)),
            dma((4,)),
        ],
        compiler_params=pltpu.CompilerParams(
            collective_id=0, has_side_effects=True, vmem_limit_bytes=VMEM_ALL - VMEM_ROOM
        ),
        name="iterate",
    )(tile_cols, tile_rows, tile_count, locked, current_block, previous_block, adjacency_tiles)
    return pl.pallas_call(
        store_kernel,
        out_shape=shapes,
        in_specs=[vmem] * 3,
        out_specs=(anywhere,) * 3,
        scratch_shapes=[dma((3,))],
        compiler_params=pltpu.CompilerParams(vmem_limit_bytes=VMEM_ALL - VMEM_ROOM),
        name="store",
    )(*results)


def solution(mesh):
    split_all = ("graphs", "rows", "cols", "sub")
    sizes = tuple(mesh.shape[name] for name in ("rows", "cols", "sub"))
    in_specs = (
        P(None, split_all),
        P(None, split_all),
        P(split_all, None, None),
        P(split_all),
        P(split_all),
        P(split_all),
        P("graphs"),
    )
    out_specs = (P(None, split_all), P(None, split_all), P("graphs", None))
    return jax.shard_map(
        functools.partial(body, sizes), mesh=mesh, in_specs=in_specs, out_specs=out_specs, check_vma=False
    )
```

```python
import functools

import jax
import jax.numpy as jnp
from jax import lax
from jax.experimental import pallas as pl
from jax.experimental.pallas import tpu as pltpu
from jax.sharding import PartitionSpec as P

MESH = pl.DeviceIdType.MESH
F32 = jnp.float32
BF16 = jnp.bfloat16
HIGHEST = lax.Precision.HIGHEST
NT_DIMS = (((1,), (1,)), ((), ()))
EDGE = 8
VMEM_ALL = 67043328
VMEM_ROOM = 10600 * 1024


def split(values):
    high = values.astype(BF16)
    return high, (values - high.astype(F32)).astype(BF16)


def iota(shape, dim):
    return lax.broadcasted_iota(jnp.int32, shape, dim)


def tree_sum(terms):
    while len(terms) > 1:
        terms = [a + b for a, b in zip(terms[::2], terms[1::2])] + terms[len(terms) & ~1 :]
    return terms[0]


def panel(matrix, k, shift, count):
    rows = [matrix[k + i : k + i + 1, :] for i in range(count)]
    columns = [
        jnp.broadcast_to(matrix[:, shift + k + i : shift + k + i + 1], matrix.shape)
        for i in range(count)
    ]
    block = {
        (i, j): jnp.broadcast_to(rows[i][:, shift + k + j : shift + k + j + 1], (1, 128))
        for i in range(count)
        for j in range(i, count)
    }
    done = []
    for m in range(count):
        inverse = 1.0 / block[m, m]
        done.append(rows[m] * lax.rsqrt(block[m, m]))
        factors = {j: block[m, j] * inverse for j in range(m + 1, count)}
        for i in range(m + 1, count):
            for j in range(i, count):
                block[i, j] = block[i, j] - factors[i] * block[m, j]
            rows[i] = rows[i] - factors[i] * rows[m]
            columns[i] = columns[i] - factors[i] * columns[m]
        matrix = matrix - columns[m] * (rows[m] * inverse)
    return matrix, done


def iterate_kernel(
    sizes, vertex_total,
    ints_hbm, x_hbm, p_hbm, tiles_hbm,
    w_ref, aw_ref, ritz_ref,
    ints_ref, index_ref, before_ref, last_ref,
    raw, halves, xh, ph, yh, q_buf, z_buf, seg, near_ref, far_ref, every, upper,
    int_sem, block_sem, tile_sem, halo_send, halo_recv, near_send, near_recv, far_send, far_recv,
    all_send, all_recv,
):
    row_count, col_count, sub_count = sizes
    near_count = col_count * sub_count
    total = row_count * near_count
    vectors, here = w_ref.shape
    slots, tile, _ = raw.shape
    row_tiles = here // tile
    reach = row_tiles // 2
    spare = slots - row_tiles
    chunk = row_tiles
    chunks = slots // chunk
    width = 3 * vectors

    row_at = lax.axis_index("rows")
    col_at = lax.axis_index("cols")
    sub_at = lax.axis_index("sub")
    position = row_at * near_count + col_at * sub_count + sub_at

    def place(spot):
        return {
            "rows": lax.div(spot, near_count),
            "cols": lax.div(lax.rem(spot, near_count), sub_count),
            "sub": lax.rem(spot, sub_count),
        }

    rows_from = [lax.rem(row_at + k, row_count) for k in range(row_count)]
    cols_from = [lax.rem(col_at + k, col_count) for k in range(col_count)]
    subs_from = [lax.rem(sub_at + k, sub_count) for k in range(sub_count)]

    def each_peer(act):
        if total <= 32:
            for k in range(1, total):
                act(
                    {
                        "rows": rows_from[k // near_count],
                        "cols": cols_from[k % near_count // sub_count],
                        "sub": subs_from[k % sub_count],
                    }
                )
        else:

            def step(k, carry):
                act(place(lax.rem(position + k, total)))
                return carry

            lax.fori_loop(1, total, step, 0)

    barrier = pltpu.get_barrier_semaphore()
    each_peer(
        lambda device: pl.semaphore_signal(barrier, inc=1, device_id=device, device_id_type=MESH)
    )

    own = pl.ds(reach, row_tiles)

    def block_start(source, target, sem):
        for t in range(row_tiles):
            pltpu.make_async_copy(
                source.at[:, pl.ds(t * tile, tile)], target.at[reach + t], sem
            ).start()

    def block_wait(target, sem):
        pltpu.make_async_copy(target.at[own], target.at[own], sem).wait()

    block_start(x_hbm, xh, block_sem.at[0])
    int_copy = pltpu.make_async_copy(ints_hbm, ints_ref, int_sem.at[0])
    int_copy.start()
    tile_copies = []
    for c in range(chunks):
        part = pl.ds(c * chunk, chunk)
        tile_copies.append(pltpu.make_async_copy(tiles_hbm.at[part], raw.at[part], tile_sem.at[c]))
    tile_copies[0].start()
    block_start(p_hbm, ph, block_sem.at[1])
    for copy in tile_copies[1:]:
        copy.start()

    has_left = position > 0
    has_right = position < total - 1
    left_device = place(lax.max(position - 1, 0))
    right_device = place(lax.min(position + 1, total - 1))

    def halo_copies(buffer, which):
        left = pltpu.make_async_remote_copy(
            src_ref=buffer.at[pl.ds(reach, reach)],
            dst_ref=buffer.at[pl.ds(reach + row_tiles, reach)],
            send_sem=halo_send.at[which, 0],
            recv_sem=halo_recv.at[which, 0],
            device_id=left_device,
            device_id_type=MESH,
        )
        right = pltpu.make_async_remote_copy(
            src_ref=buffer.at[pl.ds(row_tiles, reach)],
            dst_ref=buffer.at[pl.ds(0, reach)],
            send_sem=halo_send.at[which, 1],
            recv_sem=halo_recv.at[which, 1],
            device_id=right_device,
            device_id_type=MESH,
        )
        return left, right

    def halo_do(first_when, first, second_when, second):
        @pl.when(first_when)
        def _():
            first()

        @pl.when(second_when)
        def _():
            second()

    def halo_start(copies):
        halo_do(has_left, copies[0].start, has_right, copies[1].start)

    def halo_arrived(copies):
        halo_do(has_right, copies[0].wait_recv, has_left, copies[1].wait_recv)

    def halo_sent(copies):
        halo_do(has_left, copies[0].wait_send, has_right, copies[1].wait_send)

    x_halo = halo_copies(xh, 0)
    p_halo = halo_copies(ph, 1)
    y_halo = halo_copies(yh, 2)

    block_wait(xh, block_sem.at[0])
    pl.semaphore_wait(barrier, total - 1)
    halo_start(x_halo)

    def product(block, slot):
        high, low = split(block)
        lhs = jnp.concatenate(
            [jnp.concatenate([high, high], axis=1), jnp.concatenate([low, low], axis=1)], axis=0
        )
        out = jnp.dot(lhs, halves[slot], preferred_element_type=F32)
        return out[:vectors] + out[vectors:]

    def split_tiles(c):
        tile_copies[c].wait()

        def step(i, carry):
            for j in range(2):
                t = c * chunk + 2 * i + j
                high, low = split(raw[t])
                halves[t, 0:tile, :] = high
                halves[t, tile : 2 * tile, :] = low
            return carry

        lax.fori_loop(0, chunk // 2, step, 0)

    def diagonal(source, target, target_base):
        def step(g, carry):
            for i in range(8):
                r = g * 8 + i
                target[target_base + r] = product(source[reach + r], r)
            return carry

        lax.fori_loop(0, row_tiles // 8, step, 0)

    def tables():
        int_copy.wait()
        live = ints_ref[2 * slots]
        base_col = position * row_tiles - reach
        base_row = position * row_tiles
        at = []
        for t in range(spare):
            index_ref[t] = jnp.clip(ints_ref[row_tiles + t] - base_col, 0, 2 * row_tiles - 1)
            row = jnp.where(row_tiles + t < live, ints_ref[slots + row_tiles + t] - base_row, -1)
            link = jnp.int32(0)
            for s in range(t):
                link = jnp.where(at[s] == row, s + 1, link)
            before_ref[t] = link
            at.append(row)
        for r in range(row_tiles):
            link = jnp.int32(0)
            for s in range(spare):
                link = jnp.where(at[s] == r, s + 1, link)
            last_ref[r] = link

    def scattered(padded, target, target_base):
        for t in range(spare):
            out = product(padded[index_ref[t]], row_tiles + t)
            seg[t + 1] = out + seg[before_ref[t]]
        for r in range(row_tiles):
            target[target_base + r] = target[target_base + r] + seg[last_ref[r]]

    def parts(buffer, start):
        pieces = [split(buffer[start + t]) for t in range(row_tiles)]
        return [jnp.concatenate([piece[half] for piece in pieces], axis=1) for half in range(2)]

    def inner(left, right):
        lhs = jnp.concatenate([v[0] for v in left] + [v[1] for v in left], axis=0)
        rhs = jnp.concatenate([v[0] for v in right] + [v[1] for v in right], axis=0)
        out = lax.dot_general(lhs, rhs, NT_DIMS, preferred_element_type=F32)
        count = len(left) * vectors
        return out[:count] + out[count:]

    edge_lane = iota((EDGE, 128), 1)

    def pack(values, lanes):
        rows = values.shape[0]
        padded = jnp.concatenate([values, jnp.zeros((rows, 128 - 2 * lanes), F32)], axis=1)
        pieces = []
        for k in range(rows // EDGE):
            piece = padded[k * EDGE : (k + 1) * EDGE]
            first = piece if k == 0 else pltpu.roll(piece, k * lanes, 1)
            second = pltpu.roll(piece, (k * lanes - lanes) % 128, 1)
            here_lane = (edge_lane >= k * lanes) & (edge_lane < (k + 1) * lanes)
            pieces.append(jnp.where(here_lane, first + second, 0.0))
        return tree_sum(pieces)

    def unpack(values, rows, lanes):
        pieces = [
            values if k == 0 else pltpu.roll(values, 128 - k * lanes, 1) for k in range(rows // EDGE)
        ]
        return jnp.concatenate(pieces, axis=0)

    def stage(buffer, which, height, count, at, device, send, recv):
        def start(*values):
            mine = buffer.at[which, at, pl.ds(0, height)]
            for k, value in enumerate(values):
                buffer[which, at, k * EDGE : (k + 1) * EDGE] = value
            for k in range(1, count):
                pltpu.make_async_remote_copy(
                    src_ref=mine,
                    dst_ref=mine,
                    send_sem=send.at[which],
                    recv_sem=recv.at[which],
                    device_id=device(k),
                    device_id_type=MESH,
                ).start()

        def wait(sem):
            rest = buffer.at[which, pl.ds(0, count - 1), pl.ds(0, height)]
            pltpu.make_async_copy(rest, rest, sem.at[which]).wait()

        def collect():
            wait(recv)
            return tree_sum([buffer[which, k, 0:height] for k in range(count)])

        return start, collect, lambda: wait(send)

    def near_device(k):
        return {"cols": cols_from[k // sub_count], "sub": subs_from[k % sub_count]}

    def far_device(k):
        return {"rows": rows_from[k]}

    def any_device(k):
        return far_device(k // near_count) | near_device(k % near_count)

    near_at = col_at * sub_count + sub_at

    def near_stage(which):
        return stage(near_ref, which, EDGE, near_count, near_at, near_device, near_send, near_recv)

    def far_stage(which):
        return stage(far_ref, which, EDGE, row_count, row_at, far_device, far_send, far_recv)

    def all_stage(which):
        if total <= 32:
            return stage(every, which, EDGE, total, position, any_device, all_send, all_recv)
        first, second = near_stage(which + 1), far_stage(which + 1)

        def start(values):
            first[0](values)
            second[0](first[1]())

        def sent():
            first[2]()
            second[2]()

        return start, second[1], sent

    near_x, far_x = near_stage(0), far_stage(0)
    all_y, all_q, all_z = all_stage(0), all_stage(1), all_stage(2)

    tables()
    block_wait(ph, block_sem.at[1])
    seg[0] = jnp.zeros((vectors, tile), F32)
    for c in range(chunks):
        split_tiles(c)
        if c == row_tiles // chunk - 1:
            diagonal(xh, yh, reach)
    halo_start(p_halo)
    diagonal(ph, q_buf, 0)
    x_parts, p_parts = parts(xh, reach), parts(ph, reach)
    near_x[0](pack(inner((x_parts, p_parts), (x_parts, p_parts)), 2 * vectors))

    halo_arrived(x_halo)
    scattered(xh, yh, reach)
    halo_start(y_halo)
    y_parts = parts(yh, reach)
    basis = (x_parts, y_parts, p_parts)
    all_y[0](pack(inner(basis, (y_parts,)), vectors))

    far_x[0](near_x[1]())
    halo_arrived(p_halo)
    scattered(ph, q_buf, 0)
    all_q[0](pack(inner(basis, (parts(q_buf, 0),)), vectors))
    diagonal(yh, z_buf, 0)
    halo_arrived(y_halo)
    scattered(yh, z_buf, 0)
    all_z[0](pack(inner(basis, (parts(z_buf, 0),)), vectors))

    scale = 1.0 / vertex_total
    locked = ints_ref[2 * slots + 1]
    by_xp = unpack(far_x[1](), 2 * vectors, 2 * vectors)
    by_y = unpack(all_y[1](), width, vectors)
    lane_w = iota((vectors, 128), 1)
    line_w = iota((vectors, 128), 0)
    middle_w = (lane_w >= vectors) & (lane_w < 2 * vectors)
    shifted_y = pltpu.roll(by_y, vectors, 1)
    shifted_xp = pltpu.roll(by_xp, vectors, 1)
    on_first = lane_w == line_w
    on_second = lane_w == line_w + vectors
    free_down = iota((vectors, 1), 0) >= locked
    free_along = (iota((1, 128), 1) >= vectors + locked) & (iota((1, 128), 1) < 2 * vectors)

    def diagonal_of(mask, values, axis):
        return jnp.sum(jnp.where(mask, values, 0.0), axis=axis, keepdims=True)

    def ratio(mask, over, under, axis):
        return (diagonal_of(mask, over, axis) + 1e-06) / (diagonal_of(mask, under, axis) + 1e-06)

    down = jnp.where(free_down, ratio(on_first, by_y[:vectors], by_xp[:vectors], 1), 0.0)
    along = jnp.where(
        free_along, ratio(on_second, shifted_y[:vectors], shifted_xp[:vectors], 0), 0.0
    )

    lane = iota((width, 128), 1)
    line = iota((width, 128), 0)
    is_first = lane < vectors
    is_second = (lane >= vectors) & (lane < 2 * vectors)
    is_third = (lane >= 2 * vectors) & (lane < width)
    square = jnp.concatenate(
        [jnp.where(lane < vectors, by_y, 0.0), jnp.zeros((128 - width, 128), F32)], axis=0
    )
    y_rows = jnp.transpose(square)[:vectors]
    zero_w = jnp.zeros((vectors, 128), F32)
    over_x = jnp.concatenate([by_xp[:vectors], y_rows, by_xp[vectors:]], axis=0)
    over_x_next = jnp.concatenate(
        [shifted_xp[:vectors], pltpu.roll(y_rows, vectors, 1), shifted_xp[vectors:]], axis=0
    )
    over_p = jnp.concatenate([shifted_xp[:vectors], y_rows, shifted_xp[vectors:]], axis=0)
    gate = jnp.where(free_along, 1.0, 0.0)

    def residual_rows(values):
        first, second, third = [values[i * vectors : (i + 1) * vectors] for i in range(3)]
        return jnp.concatenate(
            [first, jnp.where(free_down, down * first - second, 0.0), third], axis=0
        )

    def three(first, second, third):
        return jnp.where(
            is_first, first, jnp.where(is_second, second, jnp.where(is_third, third, 0.0))
        )

    gram = residual_rows(
        three(over_x, over_x_next * along - shifted_y * gate, over_p)
    )
    gram = gram * scale

    rest = gram[vectors : 2 * vectors]
    frozen = on_second & (line_w < locked)
    small = jnp.where(middle_w, rest + jnp.where(frozen, 1.0, 0.0), 0.0)
    small = small + jnp.where(lane_w == line_w + 2 * vectors, 1.0, 0.0)
    padded = (line == lane) & (line >= vectors) & (line < vectors + locked)
    big = gram + jnp.where(padded | (lane == line + width), 1.0, 0.0)

    step = 4
    small_rows = []
    for k in range(0, vectors, step):
        small, done = panel(small, k, vectors, step)
        small_rows += done
    inverse_w = jnp.concatenate(small_rows, axis=0)[:, 2 * vectors : 3 * vectors]

    def outputs():
        high, low = split(inverse_w)
        lhs = jnp.concatenate(
            [jnp.concatenate([high, high], axis=1), jnp.concatenate([low, low], axis=1)], axis=0
        )

        def turn(values):
            rhs = jnp.concatenate(split(values), axis=0)
            out = jnp.dot(lhs, rhs, preferred_element_type=F32)
            return out[:vectors] + out[vectors:]

        for t in range(row_tiles):
            lanes = slice(t * tile, (t + 1) * tile)
            image = yh[reach + t]
            residual = jnp.where(free_down, down * xh[reach + t] - image, 0.0)
            carried = jnp.where(free_down, down * image - z_buf[t], 0.0)
            w_ref[:, lanes] = turn(residual)
            aw_ref[:, lanes] = turn(residual - carried)

    for k in range(0, width, step):
        if k == 2 * vectors:
            outputs()
        big, done = panel(big, k, 0, step)
        for i in range(step):
            upper[k + i : k + i + 1, :] = done[i]
    inverse = upper[:, width : 2 * width]

    by_q = unpack(all_q[1](), width, vectors)
    early = residual_rows(three(by_y, shifted_y * along, pltpu.roll(by_q, 2 * vectors, 1)))
    by_z = unpack(all_z[1](), width, vectors)
    late = residual_rows(jnp.where(is_second, pltpu.roll(by_z, vectors, 1) * gate, 0.0))
    image = (gram - scale * (early - late))[:, :width]
    half = jnp.dot(inverse, image, precision=HIGHEST, preferred_element_type=F32)
    first = lax.dot_general(half, inverse, NT_DIMS, precision=HIGHEST, preferred_element_type=F32)
    second = lax.dot_general(inverse, half, NT_DIMS, precision=HIGHEST, preferred_element_type=F32)
    ritz_ref[...] = 0.5 * (first + second)

    halo_sent(x_halo)
    halo_sent(p_halo)
    halo_sent(y_halo)
    for done in (near_x, far_x, all_y, all_q, all_z):
        done[2]()


def store_kernel(w_ref, aw_ref, ritz_ref, w_hbm, aw_hbm, ritz_hbm, sem):
    copies = [
        pltpu.make_async_copy(source, target, sem.at[i])
        for i, (source, target) in enumerate(
            ((w_ref, w_hbm), (aw_ref, aw_hbm), (ritz_ref, ritz_hbm))
        )
    ]
    for copy in copies:
        copy.start()
    for copy in copies:
        copy.wait()


def body(sizes, current_block, previous_block, adjacency_tiles, tile_rows, tile_cols, tile_count, locked):
    vectors, here = current_block.shape
    slots, tile, _ = adjacency_tiles.shape
    row_tiles = here // tile
    row_count, col_count, sub_count = sizes
    near_count = col_count * sub_count
    total = row_count * near_count
    width = 3 * vectors
    spare = slots - row_tiles
    vmem = pl.BlockSpec(memory_space=pltpu.VMEM)
    anywhere = pl.BlockSpec(memory_space=pl.ANY)
    dma = pltpu.SemaphoreType.DMA
    grid = (2 * row_tiles, vectors, tile)
    own = (row_tiles, vectors, tile)
    shapes = (
        jax.ShapeDtypeStruct((vectors, here), F32),
        jax.ShapeDtypeStruct((vectors, here), F32),
        jax.ShapeDtypeStruct((width, width), F32),
    )
    used = 2 * slots + 2
    ints = jnp.concatenate(
        [tile_cols, tile_rows, tile_count, locked, jnp.zeros((-used % 128,), jnp.int32)]
    )
    results = pl.pallas_call(
        functools.partial(iterate_kernel, sizes, here * total),
        out_shape=shapes,
        in_specs=[anywhere] * 4,
        out_specs=(vmem, vmem, vmem),
        scratch_shapes=[
            pltpu.SMEM(ints.shape, jnp.int32),
            pltpu.SMEM((spare,), jnp.int32),
            pltpu.SMEM((spare,), jnp.int32),
            pltpu.SMEM((row_tiles,), jnp.int32),
            pltpu.VMEM((slots, tile, tile), F32),
            pltpu.VMEM((slots, 2 * tile, tile), BF16),
            pltpu.VMEM(grid, F32),
            pltpu.VMEM(grid, F32),
            pltpu.VMEM(grid, F32),
            pltpu.VMEM(own, F32),
            pltpu.VMEM(own, F32),
            pltpu.VMEM((spare + 1, vectors, tile), F32),
            pltpu.VMEM((4, near_count, EDGE, 128), F32),
            pltpu.VMEM((4, row_count, EDGE, 128), F32),
            pltpu.VMEM((3, total, EDGE, 128), F32),
            pltpu.VMEM((width, 128), F32),
            dma((1,)),
            dma((2,)),
            dma((slots // row_tiles,)),
            dma((3, 2)),
            dma((3, 2)),
            dma((4,)),
            dma((4,)),
            dma((4,)),
            dma((4,)),
            dma((3,)),
            dma((3,)),
        ],
        compiler_params=pltpu.CompilerParams(
            collective_id=0, has_side_effects=True, vmem_limit_bytes=VMEM_ALL - VMEM_ROOM
        ),
        name="iterate",
    )(ints, current_block, previous_block, adjacency_tiles)
    return pl.pallas_call(
        store_kernel,
        out_shape=shapes,
        in_specs=[vmem] * 3,
        out_specs=(anywhere,) * 3,
        scratch_shapes=[dma((3,))],
        compiler_params=pltpu.CompilerParams(vmem_limit_bytes=VMEM_ALL - VMEM_ROOM),
        name="store",
    )(*results)


def solution(mesh):
    split_all = ("graphs", "rows", "cols", "sub")
    sizes = tuple(mesh.shape[name] for name in ("rows", "cols", "sub"))
    in_specs = (
        P(None, split_all),
        P(None, split_all),
        P(split_all, None, None),
        P(split_all),
        P(split_all),
        P(split_all),
        P("graphs"),
    )
    out_specs = (P(None, split_all), P(None, split_all), P("graphs", None))
    return jax.shard_map(
        functools.partial(body, sizes), mesh=mesh, in_specs=in_specs, out_specs=out_specs, check_vma=False
    )
```

```python
import functools

import jax
import jax.numpy as jnp
from jax import lax
from jax.experimental import pallas as pl
from jax.experimental.pallas import tpu as pltpu
from jax.sharding import PartitionSpec as P

MESH = pl.DeviceIdType.MESH
F32 = jnp.float32
BF16 = jnp.bfloat16
HIGHEST = lax.Precision.HIGHEST
NT_DIMS = (((1,), (1,)), ((), ()))
EDGE = 8
VMEM_ALL = 67043328
VMEM_ROOM = 10600 * 1024


def split(values):
    high = values.astype(BF16)
    return high, (values - high.astype(F32)).astype(BF16)


def iota(shape, dim):
    return lax.broadcasted_iota(jnp.int32, shape, dim)


def tree_sum(terms):
    while len(terms) > 1:
        terms = [a + b for a, b in zip(terms[::2], terms[1::2])] + terms[len(terms) & ~1 :]
    return terms[0]


def panel(matrix, k, shift, count):
    rows = [matrix[k + i : k + i + 1, :] for i in range(count)]
    columns = [
        jnp.broadcast_to(matrix[:, shift + k + i : shift + k + i + 1], matrix.shape)
        for i in range(count)
    ]
    block = {
        (i, j): jnp.broadcast_to(rows[i][:, shift + k + j : shift + k + j + 1], (1, 128))
        for i in range(count)
        for j in range(i, count)
    }
    done = []
    for m in range(count):
        inverse = 1.0 / block[m, m]
        done.append(rows[m] * lax.rsqrt(block[m, m]))
        factors = {j: block[m, j] * inverse for j in range(m + 1, count)}
        for i in range(m + 1, count):
            for j in range(i, count):
                block[i, j] = block[i, j] - factors[i] * block[m, j]
            rows[i] = rows[i] - factors[i] * rows[m]
            columns[i] = columns[i] - factors[i] * columns[m]
        matrix = matrix - columns[m] * (rows[m] * inverse)
    return matrix, done


def iterate_kernel(
    sizes, vertex_total,
    ints_hbm, x_hbm, p_hbm, tiles_hbm,
    w_ref, aw_ref, ritz_ref,
    ints_ref, index_ref, before_ref, last_ref,
    raw, halves, xh, ph, yh, q_buf, z_buf, seg, near_ref, far_ref, every, upper,
    int_sem, block_sem, tile_sem, halo_send, halo_recv, near_send, near_recv, far_send, far_recv,
    all_send, all_recv, relay,
):
    row_count, col_count, sub_count = sizes
    near_count = col_count * sub_count
    total = row_count * near_count
    vectors, here = w_ref.shape
    slots, tile, _ = raw.shape
    row_tiles = here // tile
    reach = row_tiles // 2
    spare = slots - row_tiles
    chunk = row_tiles
    chunks = slots // chunk
    width = 3 * vectors

    row_at = lax.axis_index("rows")
    col_at = lax.axis_index("cols")
    sub_at = lax.axis_index("sub")
    position = row_at * near_count + col_at * sub_count + sub_at

    def place(spot):
        return {
            "rows": lax.div(spot, near_count),
            "cols": lax.div(lax.rem(spot, near_count), sub_count),
            "sub": lax.rem(spot, sub_count),
        }

    rows_from = [lax.rem(row_at + k, row_count) for k in range(row_count)]
    cols_from = [lax.rem(col_at + k, col_count) for k in range(col_count)]
    subs_from = [lax.rem(sub_at + k, sub_count) for k in range(sub_count)]

    has_left = position > 0
    has_right = position < total - 1
    has_under = row_at > 0
    has_over = row_at < row_count - 1
    left_device = place(lax.max(position - 1, 0))
    right_device = place(lax.min(position + 1, total - 1))
    under_device = {"rows": lax.max(row_at - 1, 0)}
    over_device = {"rows": lax.min(row_at + 1, row_count - 1)}
    near_at = col_at * sub_count + sub_at
    crosses_left = has_left & (near_at == 0)
    crosses_right = has_right & (near_at == near_count - 1)

    def near_device(k):
        return {"cols": cols_from[k // sub_count], "sub": subs_from[k % sub_count]}

    def far_device(k):
        return {"rows": rows_from[k]}

    def any_device(k):
        return far_device(k // near_count) | near_device(k % near_count)

    def signal(semaphore, device):
        pl.semaphore_signal(semaphore, inc=1, device_id=device, device_id_type=MESH)

    barrier = pltpu.get_barrier_semaphore()
    greeted = near_count - 1
    for there, device in (
        (crosses_left, left_device),
        (crosses_right, right_device),
        (has_under, under_device),
        (has_over, over_device),
    ):
        pl.when(there)(functools.partial(signal, barrier, device))
        greeted = greeted + jnp.where(there, 1, 0)
    for k in range(1, near_count):
        signal(barrier, near_device(k))

    def tell():
        pl.when(has_under)(functools.partial(signal, relay.at[1], under_device))
        pl.when(has_over)(functools.partial(signal, relay.at[0], over_device))

    def hear():
        pl.when(has_under)(lambda: pl.semaphore_wait(relay.at[0], 1))
        pl.when(has_over)(lambda: pl.semaphore_wait(relay.at[1], 1))

    def hear_rest():
        hear()

        def step(k, carry):
            tell()
            hear()
            return carry

        if row_count > 4:
            lax.fori_loop(0, row_count - 4, step, 0)

    own = pl.ds(reach, row_tiles)

    def block_start(source, target, sem):
        for t in range(row_tiles):
            pltpu.make_async_copy(
                source.at[:, pl.ds(t * tile, tile)], target.at[reach + t], sem
            ).start()

    def block_wait(target, sem):
        pltpu.make_async_copy(target.at[own], target.at[own], sem).wait()

    block_start(x_hbm, xh, block_sem.at[0])
    int_copy = pltpu.make_async_copy(ints_hbm, ints_ref, int_sem.at[0])
    int_copy.start()
    tile_copies = []
    for c in range(chunks):
        part = pl.ds(c * chunk, chunk)
        tile_copies.append(pltpu.make_async_copy(tiles_hbm.at[part], raw.at[part], tile_sem.at[c]))
    tile_copies[0].start()
    block_start(p_hbm, ph, block_sem.at[1])
    for copy in tile_copies[1:]:
        copy.start()

    def halo_copies(buffer, which):
        left = pltpu.make_async_remote_copy(
            src_ref=buffer.at[pl.ds(reach, reach)],
            dst_ref=buffer.at[pl.ds(reach + row_tiles, reach)],
            send_sem=halo_send.at[which, 0],
            recv_sem=halo_recv.at[which, 0],
            device_id=left_device,
            device_id_type=MESH,
        )
        right = pltpu.make_async_remote_copy(
            src_ref=buffer.at[pl.ds(row_tiles, reach)],
            dst_ref=buffer.at[pl.ds(0, reach)],
            send_sem=halo_send.at[which, 1],
            recv_sem=halo_recv.at[which, 1],
            device_id=right_device,
            device_id_type=MESH,
        )
        return left, right

    def halo_do(first_when, first, second_when, second):
        @pl.when(first_when)
        def _():
            first()

        @pl.when(second_when)
        def _():
            second()

    def halo_start(copies):
        halo_do(has_left, copies[0].start, has_right, copies[1].start)

    def halo_arrived(copies):
        halo_do(has_right, copies[0].wait_recv, has_left, copies[1].wait_recv)

    def halo_sent(copies):
        halo_do(has_left, copies[0].wait_send, has_right, copies[1].wait_send)

    x_halo = halo_copies(xh, 0)
    p_halo = halo_copies(ph, 1)
    y_halo = halo_copies(yh, 2)

    block_wait(xh, block_sem.at[0])
    pl.semaphore_wait(barrier, greeted)
    halo_start(x_halo)
    tell()

    def product(block, slot):
        high, low = split(block)
        lhs = jnp.concatenate(
            [jnp.concatenate([high, high], axis=1), jnp.concatenate([low, low], axis=1)], axis=0
        )
        out = jnp.dot(lhs, halves[slot], preferred_element_type=F32)
        return out[:vectors] + out[vectors:]

    def split_tiles(c):
        tile_copies[c].wait()

        def step(i, carry):
            for j in range(2):
                t = c * chunk + 2 * i + j
                high, low = split(raw[t])
                halves[t, 0:tile, :] = high
                halves[t, tile : 2 * tile, :] = low
            return carry

        lax.fori_loop(0, chunk // 2, step, 0)

    def diagonal(source, target, target_base):
        def step(g, carry):
            for i in range(8):
                r = g * 8 + i
                target[target_base + r] = product(source[reach + r], r)
            return carry

        lax.fori_loop(0, row_tiles // 8, step, 0)

    def tables():
        int_copy.wait()
        live = ints_ref[2 * slots]
        base_col = position * row_tiles - reach
        base_row = position * row_tiles
        at = []
        for t in range(spare):
            index_ref[t] = jnp.clip(ints_ref[row_tiles + t] - base_col, 0, 2 * row_tiles - 1)
            row = jnp.where(row_tiles + t < live, ints_ref[slots + row_tiles + t] - base_row, -1)
            link = jnp.int32(0)
            for s in range(t):
                link = jnp.where(at[s] == row, s + 1, link)
            before_ref[t] = link
            at.append(row)
        for r in range(row_tiles):
            link = jnp.int32(0)
            for s in range(spare):
                link = jnp.where(at[s] == r, s + 1, link)
            last_ref[r] = link

    def scattered(padded, target, target_base):
        for t in range(spare):
            out = product(padded[index_ref[t]], row_tiles + t)
            seg[t + 1] = out + seg[before_ref[t]]
        for r in range(row_tiles):
            target[target_base + r] = target[target_base + r] + seg[last_ref[r]]

    def parts(buffer, start):
        pieces = [split(buffer[start + t]) for t in range(row_tiles)]
        return [jnp.concatenate([piece[half] for piece in pieces], axis=1) for half in range(2)]

    def inner(left, right):
        lhs = jnp.concatenate([v[0] for v in left] + [v[1] for v in left], axis=0)
        rhs = jnp.concatenate([v[0] for v in right] + [v[1] for v in right], axis=0)
        out = lax.dot_general(lhs, rhs, NT_DIMS, preferred_element_type=F32)
        count = len(left) * vectors
        return out[:count] + out[count:]

    edge_lane = iota((EDGE, 128), 1)

    def pack(values, lanes):
        rows = values.shape[0]
        padded = jnp.concatenate([values, jnp.zeros((rows, 128 - 2 * lanes), F32)], axis=1)
        pieces = []
        for k in range(rows // EDGE):
            piece = padded[k * EDGE : (k + 1) * EDGE]
            first = piece if k == 0 else pltpu.roll(piece, k * lanes, 1)
            second = pltpu.roll(piece, (k * lanes - lanes) % 128, 1)
            here_lane = (edge_lane >= k * lanes) & (edge_lane < (k + 1) * lanes)
            pieces.append(jnp.where(here_lane, first + second, 0.0))
        return tree_sum(pieces)

    def unpack(values, rows, lanes):
        pieces = [
            values if k == 0 else pltpu.roll(values, 128 - k * lanes, 1) for k in range(rows // EDGE)
        ]
        return jnp.concatenate(pieces, axis=0)

    def stage(buffer, which, height, count, at, device, send, recv):
        def start(*values):
            mine = buffer.at[which, at, pl.ds(0, height)]
            for k, value in enumerate(values):
                buffer[which, at, k * EDGE : (k + 1) * EDGE] = value
            for k in range(1, count):
                pltpu.make_async_remote_copy(
                    src_ref=mine,
                    dst_ref=mine,
                    send_sem=send.at[which],
                    recv_sem=recv.at[which],
                    device_id=device(k),
                    device_id_type=MESH,
                ).start()

        def wait(sem):
            rest = buffer.at[which, pl.ds(0, count - 1), pl.ds(0, height)]
            pltpu.make_async_copy(rest, rest, sem.at[which]).wait()

        def collect():
            wait(recv)
            return tree_sum([buffer[which, k, 0:height] for k in range(count)])

        return start, collect, lambda: wait(send)

    def near_stage(which):
        return stage(near_ref, which, EDGE, near_count, near_at, near_device, near_send, near_recv)

    def far_stage(which):
        return stage(far_ref, which, EDGE, row_count, row_at, far_device, far_send, far_recv)

    def all_stage(which):
        if total <= 32:
            return stage(every, which, EDGE, total, position, any_device, all_send, all_recv)
        first, second = near_stage(which + 1), far_stage(which + 1)

        def start(values):
            first[0](values)
            second[0](first[1]())

        def sent():
            first[2]()
            second[2]()

        return start, second[1], sent

    near_x, far_x = near_stage(0), far_stage(0)
    all_y, all_q, all_z = all_stage(0), all_stage(1), all_stage(2)

    tables()
    hear()
    tell()
    block_wait(ph, block_sem.at[1])
    seg[0] = jnp.zeros((vectors, tile), F32)
    for c in range(chunks):
        split_tiles(c)
        if c == row_tiles // chunk - 1:
            diagonal(xh, yh, reach)
    hear()
    tell()
    halo_start(p_halo)
    diagonal(ph, q_buf, 0)
    x_parts, p_parts = parts(xh, reach), parts(ph, reach)
    near_x[0](pack(inner((x_parts, p_parts), (x_parts, p_parts)), 2 * vectors))

    hear_rest()
    halo_arrived(x_halo)
    scattered(xh, yh, reach)
    halo_start(y_halo)
    y_parts = parts(yh, reach)
    basis = (x_parts, y_parts, p_parts)
    all_y[0](pack(inner(basis, (y_parts,)), vectors))

    far_x[0](near_x[1]())
    halo_arrived(p_halo)
    scattered(ph, q_buf, 0)
    all_q[0](pack(inner(basis, (parts(q_buf, 0),)), vectors))
    diagonal(yh, z_buf, 0)
    halo_arrived(y_halo)
    scattered(yh, z_buf, 0)
    all_z[0](pack(inner(basis, (parts(z_buf, 0),)), vectors))

    scale = 1.0 / vertex_total
    locked = ints_ref[2 * slots + 1]
    by_xp = unpack(far_x[1](), 2 * vectors, 2 * vectors)
    by_y = unpack(all_y[1](), width, vectors)
    lane_w = iota((vectors, 128), 1)
    line_w = iota((vectors, 128), 0)
    middle_w = (lane_w >= vectors) & (lane_w < 2 * vectors)
    shifted_y = pltpu.roll(by_y, vectors, 1)
    shifted_xp = pltpu.roll(by_xp, vectors, 1)
    on_first = lane_w == line_w
    on_second = lane_w == line_w + vectors
    free_down = iota((vectors, 1), 0) >= locked
    free_along = (iota((1, 128), 1) >= vectors + locked) & (iota((1, 128), 1) < 2 * vectors)

    def diagonal_of(mask, values, axis):
        return jnp.sum(jnp.where(mask, values, 0.0), axis=axis, keepdims=True)

    def ratio(mask, over, under, axis):
        return (diagonal_of(mask, over, axis) + 1e-06) / (diagonal_of(mask, under, axis) + 1e-06)

    down = jnp.where(free_down, ratio(on_first, by_y[:vectors], by_xp[:vectors], 1), 0.0)
    along = jnp.where(
        free_along, ratio(on_second, shifted_y[:vectors], shifted_xp[:vectors], 0), 0.0
    )

    lane = iota((width, 128), 1)
    line = iota((width, 128), 0)
    is_first = lane < vectors
    is_second = (lane >= vectors) & (lane < 2 * vectors)
    is_third = (lane >= 2 * vectors) & (lane < width)
    square = jnp.concatenate(
        [jnp.where(lane < vectors, by_y, 0.0), jnp.zeros((128 - width, 128), F32)], axis=0
    )
    y_rows = jnp.transpose(square)[:vectors]
    zero_w = jnp.zeros((vectors, 128), F32)
    over_x = jnp.concatenate([by_xp[:vectors], y_rows, by_xp[vectors:]], axis=0)
    over_x_next = jnp.concatenate(
        [shifted_xp[:vectors], pltpu.roll(y_rows, vectors, 1), shifted_xp[vectors:]], axis=0
    )
    over_p = jnp.concatenate([shifted_xp[:vectors], y_rows, shifted_xp[vectors:]], axis=0)
    gate = jnp.where(free_along, 1.0, 0.0)

    def residual_rows(values):
        first, second, third = [values[i * vectors : (i + 1) * vectors] for i in range(3)]
        return jnp.concatenate(
            [first, jnp.where(free_down, down * first - second, 0.0), third], axis=0
        )

    def three(first, second, third):
        return jnp.where(
            is_first, first, jnp.where(is_second, second, jnp.where(is_third, third, 0.0))
        )

    gram = residual_rows(
        three(over_x, over_x_next * along - shifted_y * gate, over_p)
    )
    gram = gram * scale

    rest = gram[vectors : 2 * vectors]
    frozen = on_second & (line_w < locked)
    small = jnp.where(middle_w, rest + jnp.where(frozen, 1.0, 0.0), 0.0)
    small = small + jnp.where(lane_w == line_w + 2 * vectors, 1.0, 0.0)
    padded = (line == lane) & (line >= vectors) & (line < vectors + locked)
    big = gram + jnp.where(padded | (lane == line + width), 1.0, 0.0)

    step = 4
    small_rows = []
    for k in range(0, vectors, step):
        small, done = panel(small, k, vectors, step)
        small_rows += done
    inverse_w = jnp.concatenate(small_rows, axis=0)[:, 2 * vectors : 3 * vectors]

    def outputs():
        high, low = split(inverse_w)
        lhs = jnp.concatenate(
            [jnp.concatenate([high, high], axis=1), jnp.concatenate([low, low], axis=1)], axis=0
        )

        def turn(values):
            rhs = jnp.concatenate(split(values), axis=0)
            out = jnp.dot(lhs, rhs, preferred_element_type=F32)
            return out[:vectors] + out[vectors:]

        for t in range(row_tiles):
            lanes = slice(t * tile, (t + 1) * tile)
            image = yh[reach + t]
            residual = jnp.where(free_down, down * xh[reach + t] - image, 0.0)
            carried = jnp.where(free_down, down * image - z_buf[t], 0.0)
            w_ref[:, lanes] = turn(residual)
            aw_ref[:, lanes] = turn(residual - carried)

    for k in range(0, width, step):
        if k == 2 * vectors:
            outputs()
        big, done = panel(big, k, 0, step)
        for i in range(step):
            upper[k + i : k + i + 1, :] = done[i]
    inverse = upper[:, width : 2 * width]

    by_q = unpack(all_q[1](), width, vectors)
    early = residual_rows(three(by_y, shifted_y * along, pltpu.roll(by_q, 2 * vectors, 1)))
    by_z = unpack(all_z[1](), width, vectors)
    late = residual_rows(jnp.where(is_second, pltpu.roll(by_z, vectors, 1) * gate, 0.0))
    image = (gram - scale * (early - late))[:, :width]
    half = jnp.dot(inverse, image, precision=HIGHEST, preferred_element_type=F32)
    first = lax.dot_general(half, inverse, NT_DIMS, precision=HIGHEST, preferred_element_type=F32)
    second = lax.dot_general(inverse, half, NT_DIMS, precision=HIGHEST, preferred_element_type=F32)
    ritz_ref[...] = 0.5 * (first + second)

    halo_sent(x_halo)
    halo_sent(p_halo)
    halo_sent(y_halo)
    for done in (near_x, far_x, all_y, all_q, all_z):
        done[2]()


def store_kernel(w_ref, aw_ref, ritz_ref, w_hbm, aw_hbm, ritz_hbm, sem):
    copies = [
        pltpu.make_async_copy(source, target, sem.at[i])
        for i, (source, target) in enumerate(
            ((w_ref, w_hbm), (aw_ref, aw_hbm), (ritz_ref, ritz_hbm))
        )
    ]
    for copy in copies:
        copy.start()
    for copy in copies:
        copy.wait()


def body(sizes, current_block, previous_block, adjacency_tiles, tile_rows, tile_cols, tile_count, locked):
    vectors, here = current_block.shape
    slots, tile, _ = adjacency_tiles.shape
    row_tiles = here // tile
    row_count, col_count, sub_count = sizes
    near_count = col_count * sub_count
    total = row_count * near_count
    width = 3 * vectors
    spare = slots - row_tiles
    vmem = pl.BlockSpec(memory_space=pltpu.VMEM)
    anywhere = pl.BlockSpec(memory_space=pl.ANY)
    dma = pltpu.SemaphoreType.DMA
    grid = (2 * row_tiles, vectors, tile)
    own = (row_tiles, vectors, tile)
    shapes = (
        jax.ShapeDtypeStruct((vectors, here), F32),
        jax.ShapeDtypeStruct((vectors, here), F32),
        jax.ShapeDtypeStruct((width, width), F32),
    )
    used = 2 * slots + 2
    ints = jnp.concatenate(
        [tile_cols, tile_rows, tile_count, locked, jnp.zeros((-used % 128,), jnp.int32)]
    )
    results = pl.pallas_call(
        functools.partial(iterate_kernel, sizes, here * total),
        out_shape=shapes,
        in_specs=[anywhere] * 4,
        out_specs=(vmem, vmem, vmem),
        scratch_shapes=[
            pltpu.SMEM(ints.shape, jnp.int32),
            pltpu.SMEM((spare,), jnp.int32),
            pltpu.SMEM((spare,), jnp.int32),
            pltpu.SMEM((row_tiles,), jnp.int32),
            pltpu.VMEM((slots, tile, tile), F32),
            pltpu.VMEM((slots, 2 * tile, tile), BF16),
            pltpu.VMEM(grid, F32),
            pltpu.VMEM(grid, F32),
            pltpu.VMEM(grid, F32),
            pltpu.VMEM(own, F32),
            pltpu.VMEM(own, F32),
            pltpu.VMEM((spare + 1, vectors, tile), F32),
            pltpu.VMEM((4, near_count, EDGE, 128), F32),
            pltpu.VMEM((4, row_count, EDGE, 128), F32),
            pltpu.VMEM((3, total, EDGE, 128), F32),
            pltpu.VMEM((width, 128), F32),
            dma((1,)),
            dma((2,)),
            dma((slots // row_tiles,)),
            dma((3, 2)),
            dma((3, 2)),
            dma((4,)),
            dma((4,)),
            dma((4,)),
            dma((4,)),
            dma((3,)),
            dma((3,)),
            pltpu.SemaphoreType.REGULAR((2,)),
        ],
        compiler_params=pltpu.CompilerParams(
            collective_id=0, has_side_effects=True, vmem_limit_bytes=VMEM_ALL - VMEM_ROOM
        ),
        name="iterate",
    )(ints, current_block, previous_block, adjacency_tiles)
    return pl.pallas_call(
        store_kernel,
        out_shape=shapes,
        in_specs=[vmem] * 3,
        out_specs=(anywhere,) * 3,
        scratch_shapes=[dma((3,))],
        compiler_params=pltpu.CompilerParams(vmem_limit_bytes=VMEM_ALL - VMEM_ROOM),
        name="store",
    )(*results)


def solution(mesh):
    split_all = ("graphs", "rows", "cols", "sub")
    sizes = tuple(mesh.shape[name] for name in ("rows", "cols", "sub"))
    in_specs = (
        P(None, split_all),
        P(None, split_all),
        P(split_all, None, None),
        P(split_all),
        P(split_all),
        P(split_all),
        P("graphs"),
    )
    out_specs = (P(None, split_all), P(None, split_all), P("graphs", None))
    return jax.shard_map(
        functools.partial(body, sizes), mesh=mesh, in_specs=in_specs, out_specs=out_specs, check_vma=False
    )
```

```python
import functools

import jax
import jax.numpy as jnp
from jax import lax
from jax.experimental import pallas as pl
from jax.experimental.pallas import tpu as pltpu
from jax.sharding import PartitionSpec as P

MESH = pl.DeviceIdType.MESH
F32 = jnp.float32
BF16 = jnp.bfloat16
HIGHEST = lax.Precision.HIGHEST
NT_DIMS = (((1,), (1,)), ((), ()))
EDGE = 8
VMEM_ALL = 67043328
VMEM_ROOM = 10600 * 1024


def split(values):
    high = values.astype(BF16)
    return high, (values - high.astype(F32)).astype(BF16)


def iota(shape, dim):
    return lax.broadcasted_iota(jnp.int32, shape, dim)


def tree_sum(terms):
    while len(terms) > 1:
        terms = [a + b for a, b in zip(terms[::2], terms[1::2])] + terms[len(terms) & ~1 :]
    return terms[0]


def panel(matrix, k, shift, count):
    rows = [matrix[k + i : k + i + 1, :] for i in range(count)]
    columns = [
        jnp.broadcast_to(matrix[:, shift + k + i : shift + k + i + 1], matrix.shape)
        for i in range(count)
    ]
    block = {
        (i, j): jnp.broadcast_to(rows[i][:, shift + k + j : shift + k + j + 1], (1, 128))
        for i in range(count)
        for j in range(i, count)
    }
    done = []
    for m in range(count):
        inverse = 1.0 / block[m, m]
        done.append(rows[m] * lax.rsqrt(block[m, m]))
        factors = {j: block[m, j] * inverse for j in range(m + 1, count)}
        for i in range(m + 1, count):
            for j in range(i, count):
                block[i, j] = block[i, j] - factors[i] * block[m, j]
            rows[i] = rows[i] - factors[i] * rows[m]
            columns[i] = columns[i] - factors[i] * columns[m]
        matrix = matrix - columns[m] * (rows[m] * inverse)
    return matrix, done


def iterate_kernel(
    sizes, vertex_total,
    ints_hbm, x_hbm, p_hbm, tiles_hbm,
    w_ref, aw_ref, ritz_ref,
    ints_ref, index_ref, before_ref, last_ref,
    raw, halves, xh, ph, yh, q_buf, z_buf, seg, near_ref, far_ref, every, upper,
    int_sem, block_sem, tile_sem, halo_send, halo_recv, near_send, near_recv, far_send, far_recv,
    all_send, all_recv, relay,
):
    row_count, col_count, sub_count = sizes
    near_count = col_count * sub_count
    total = row_count * near_count
    vectors, here = w_ref.shape
    slots, tile, _ = raw.shape
    row_tiles = here // tile
    reach = row_tiles // 2
    spare = slots - row_tiles
    chunk = row_tiles
    chunks = slots // chunk
    width = 3 * vectors

    row_at = lax.axis_index("rows")
    col_at = lax.axis_index("cols")
    sub_at = lax.axis_index("sub")
    position = row_at * near_count + col_at * sub_count + sub_at

    def place(spot):
        return {
            "rows": lax.div(spot, near_count),
            "cols": lax.div(lax.rem(spot, near_count), sub_count),
            "sub": lax.rem(spot, sub_count),
        }

    rows_from = [lax.rem(row_at + k, row_count) for k in range(row_count)]
    cols_from = [lax.rem(col_at + k, col_count) for k in range(col_count)]
    subs_from = [lax.rem(sub_at + k, sub_count) for k in range(sub_count)]

    has_left = position > 0
    has_right = position < total - 1
    has_under = row_at > 0
    has_over = row_at < row_count - 1
    left_device = place(lax.max(position - 1, 0))
    right_device = place(lax.min(position + 1, total - 1))
    under_device = {"rows": lax.max(row_at - 1, 0)}
    over_device = {"rows": lax.min(row_at + 1, row_count - 1)}
    near_at = col_at * sub_count + sub_at
    crosses_left = has_left & (near_at == 0)
    crosses_right = has_right & (near_at == near_count - 1)

    def near_device(k):
        return {"cols": cols_from[k // sub_count], "sub": subs_from[k % sub_count]}

    def far_device(k):
        return {"rows": rows_from[k]}

    def any_device(k):
        turn = (k - 1) // near_count
        if turn == row_count - 1:
            return near_device(k - turn * near_count)
        up = turn + jnp.where(turn >= row_at, 1, 0)
        down = row_count - 1 - turn
        down = down - jnp.where(down <= row_at, 1, 0)
        return {"rows": jnp.where(2 * row_at >= row_count, up, down)} | near_device((k - 1) % near_count)

    def signal(semaphore, device):
        pl.semaphore_signal(semaphore, inc=1, device_id=device, device_id_type=MESH)

    barrier = pltpu.get_barrier_semaphore()
    greeted = near_count - 1
    for there, device in (
        (crosses_left, left_device),
        (crosses_right, right_device),
        (has_under, under_device),
        (has_over, over_device),
    ):
        pl.when(there)(functools.partial(signal, barrier, device))
        greeted = greeted + jnp.where(there, 1, 0)
    for k in range(1, near_count):
        signal(barrier, near_device(k))

    def tell():
        pl.when(has_under)(functools.partial(signal, relay.at[1], under_device))
        pl.when(has_over)(functools.partial(signal, relay.at[0], over_device))

    def hear():
        pl.when(has_under)(lambda: pl.semaphore_wait(relay.at[0], 1))
        pl.when(has_over)(lambda: pl.semaphore_wait(relay.at[1], 1))

    def hear_rest():
        hear()

        def step(k, carry):
            tell()
            hear()
            return carry

        if row_count > 4:
            lax.fori_loop(0, row_count - 4, step, 0)

    own = pl.ds(reach, row_tiles)

    def block_start(source, target, sem):
        for t in range(row_tiles):
            pltpu.make_async_copy(
                source.at[:, pl.ds(t * tile, tile)], target.at[reach + t], sem
            ).start()

    def block_wait(target, sem):
        pltpu.make_async_copy(target.at[own], target.at[own], sem).wait()

    block_start(x_hbm, xh, block_sem.at[0])
    int_copy = pltpu.make_async_copy(ints_hbm, ints_ref, int_sem.at[0])
    int_copy.start()
    tile_copies = []
    for c in range(chunks):
        part = pl.ds(c * chunk, chunk)
        tile_copies.append(pltpu.make_async_copy(tiles_hbm.at[part], raw.at[part], tile_sem.at[c]))
    tile_copies[0].start()
    block_start(p_hbm, ph, block_sem.at[1])
    for copy in tile_copies[1:]:
        copy.start()

    def halo_copies(buffer, which):
        left = pltpu.make_async_remote_copy(
            src_ref=buffer.at[pl.ds(reach, reach)],
            dst_ref=buffer.at[pl.ds(reach + row_tiles, reach)],
            send_sem=halo_send.at[which, 0],
            recv_sem=halo_recv.at[which, 0],
            device_id=left_device,
            device_id_type=MESH,
        )
        right = pltpu.make_async_remote_copy(
            src_ref=buffer.at[pl.ds(row_tiles, reach)],
            dst_ref=buffer.at[pl.ds(0, reach)],
            send_sem=halo_send.at[which, 1],
            recv_sem=halo_recv.at[which, 1],
            device_id=right_device,
            device_id_type=MESH,
        )
        return left, right

    def halo_do(first_when, first, second_when, second):
        @pl.when(first_when)
        def _():
            first()

        @pl.when(second_when)
        def _():
            second()

    def halo_start(copies):
        halo_do(has_left, copies[0].start, has_right, copies[1].start)

    def halo_arrived(copies):
        halo_do(has_right, copies[0].wait_recv, has_left, copies[1].wait_recv)

    def halo_sent(copies):
        halo_do(has_left, copies[0].wait_send, has_right, copies[1].wait_send)

    x_halo = halo_copies(xh, 0)
    p_halo = halo_copies(ph, 1)
    y_halo = halo_copies(yh, 2)

    block_wait(xh, block_sem.at[0])
    pl.semaphore_wait(barrier, greeted)
    halo_start(x_halo)
    tell()

    def product(block, slot):
        high, low = split(block)
        lhs = jnp.concatenate(
            [jnp.concatenate([high, high], axis=1), jnp.concatenate([low, low], axis=1)], axis=0
        )
        out = jnp.dot(lhs, halves[slot], preferred_element_type=F32)
        return out[:vectors] + out[vectors:]

    def split_tiles(c):
        tile_copies[c].wait()

        def step(i, carry):
            for j in range(2):
                t = c * chunk + 2 * i + j
                high, low = split(raw[t])
                halves[t, 0:tile, :] = high
                halves[t, tile : 2 * tile, :] = low
            return carry

        lax.fori_loop(0, chunk // 2, step, 0)

    def diagonal(source, target, target_base):
        def step(g, carry):
            for i in range(8):
                r = g * 8 + i
                target[target_base + r] = product(source[reach + r], r)
            return carry

        lax.fori_loop(0, row_tiles // 8, step, 0)

    def tables():
        int_copy.wait()
        live = ints_ref[2 * slots]
        base_col = position * row_tiles - reach
        base_row = position * row_tiles
        at = []
        for t in range(spare):
            index_ref[t] = jnp.clip(ints_ref[row_tiles + t] - base_col, 0, 2 * row_tiles - 1)
            row = jnp.where(row_tiles + t < live, ints_ref[slots + row_tiles + t] - base_row, -1)
            link = jnp.int32(0)
            for s in range(t):
                link = jnp.where(at[s] == row, s + 1, link)
            before_ref[t] = link
            at.append(row)
        for r in range(row_tiles):
            link = jnp.int32(0)
            for s in range(spare):
                link = jnp.where(at[s] == r, s + 1, link)
            last_ref[r] = link

    def scattered(padded, target, target_base):
        for t in range(spare):
            out = product(padded[index_ref[t]], row_tiles + t)
            seg[t + 1] = out + seg[before_ref[t]]
        for r in range(row_tiles):
            target[target_base + r] = target[target_base + r] + seg[last_ref[r]]

    def parts(buffer, start):
        pieces = [split(buffer[start + t]) for t in range(row_tiles)]
        return [jnp.concatenate([piece[half] for piece in pieces], axis=1) for half in range(2)]

    def inner(left, right):
        lhs = jnp.concatenate([v[0] for v in left] + [v[1] for v in left], axis=0)
        rhs = jnp.concatenate([v[0] for v in right] + [v[1] for v in right], axis=0)
        half = here // 2
        out = [
            lax.dot_general(lhs[:, part], rhs[:, part], NT_DIMS, preferred_element_type=F32)
            for part in (slice(0, half), slice(half, here))
        ]
        count = len(left) * vectors
        return (out[0][:count] + out[1][:count]) + (out[0][count:] + out[1][count:])

    edge_lane = iota((EDGE, 128), 1)

    def pack(values, lanes):
        rows = values.shape[0]
        padded = jnp.concatenate([values, jnp.zeros((rows, 128 - 2 * lanes), F32)], axis=1)
        pieces = []
        for k in range(rows // EDGE):
            piece = padded[k * EDGE : (k + 1) * EDGE]
            first = piece if k == 0 else pltpu.roll(piece, k * lanes, 1)
            second = pltpu.roll(piece, (k * lanes - lanes) % 128, 1)
            here_lane = (edge_lane >= k * lanes) & (edge_lane < (k + 1) * lanes)
            pieces.append(jnp.where(here_lane, first + second, 0.0))
        return tree_sum(pieces)

    def unpack(values, rows, lanes, at=0):
        pieces = [
            values if k * lanes == at else pltpu.roll(values, (at - k * lanes) % 128, 1)
            for k in range(rows // EDGE)
        ]
        return jnp.concatenate(pieces, axis=0)

    def stage(buffer, which, height, count, at, device, send, recv):
        def start(*values):
            mine = buffer.at[which, at, pl.ds(0, height)]
            for k, value in enumerate(values):
                buffer[which, at, k * EDGE : (k + 1) * EDGE] = value
            for k in range(1, count):
                pltpu.make_async_remote_copy(
                    src_ref=mine,
                    dst_ref=mine,
                    send_sem=send.at[which],
                    recv_sem=recv.at[which],
                    device_id=device(k),
                    device_id_type=MESH,
                ).start()

        def wait(sem):
            rest = buffer.at[which, pl.ds(0, count - 1), pl.ds(0, height)]
            pltpu.make_async_copy(rest, rest, sem.at[which]).wait()

        def collect():
            wait(recv)
            return tree_sum([buffer[which, k, 0:height] for k in range(count)])

        return start, collect, lambda: wait(send)

    def near_stage(which):
        return stage(near_ref, which, EDGE, near_count, near_at, near_device, near_send, near_recv)

    def far_stage(which):
        return stage(far_ref, which, EDGE, row_count, row_at, far_device, far_send, far_recv)

    def all_stage(which):
        if total <= 32:
            return stage(every, which, EDGE, total, position, any_device, all_send, all_recv)
        first, second = near_stage(which + 1), far_stage(which + 1)

        def start(values):
            first[0](values)
            second[0](first[1]())

        def sent():
            first[2]()
            second[2]()

        return start, second[1], sent

    near_x, far_x = near_stage(0), far_stage(0)
    all_y, all_q, all_z = all_stage(0), all_stage(1), all_stage(2)

    tables()
    hear()
    tell()
    block_wait(ph, block_sem.at[1])
    seg[0] = jnp.zeros((vectors, tile), F32)
    for c in range(chunks):
        split_tiles(c)
        if c == row_tiles // chunk - 1:
            diagonal(xh, yh, reach)
    hear()
    tell()
    halo_start(p_halo)
    diagonal(ph, q_buf, 0)
    x_parts, p_parts = parts(xh, reach), parts(ph, reach)
    near_x[0](pack(inner((x_parts, p_parts), (x_parts, p_parts)), 2 * vectors))

    hear_rest()
    halo_arrived(x_halo)
    scattered(xh, yh, reach)
    halo_start(y_halo)
    y_parts = parts(yh, reach)
    basis = (x_parts, y_parts, p_parts)
    all_y[0](pack(inner(basis, (y_parts,)), vectors))

    far_x[0](near_x[1]())
    halo_arrived(p_halo)
    scattered(ph, q_buf, 0)
    all_q[0](pack(inner(basis, (parts(q_buf, 0),)), vectors))
    diagonal(yh, z_buf, 0)
    halo_arrived(y_halo)
    scattered(yh, z_buf, 0)
    all_z[0](pack(inner(basis, (parts(z_buf, 0),)), vectors))

    scale = 1.0 / vertex_total
    locked = ints_ref[2 * slots + 1]
    by_xp = unpack(far_x[1](), 2 * vectors, 2 * vectors)
    by_y = unpack(all_y[1](), width, vectors)
    lane_w = iota((vectors, 128), 1)
    line_w = iota((vectors, 128), 0)
    middle_w = (lane_w >= vectors) & (lane_w < 2 * vectors)
    shifted_y = pltpu.roll(by_y, vectors, 1)
    shifted_xp = pltpu.roll(by_xp, vectors, 1)
    on_first = lane_w == line_w
    on_second = lane_w == line_w + vectors
    free_down = iota((vectors, 1), 0) >= locked
    free_along = (iota((1, 128), 1) >= vectors + locked) & (iota((1, 128), 1) < 2 * vectors)

    def diagonal_of(mask, values, axis):
        return jnp.sum(jnp.where(mask, values, 0.0), axis=axis, keepdims=True)

    def ratio(mask, over, under, axis):
        return (diagonal_of(mask, over, axis) + 1e-06) / (diagonal_of(mask, under, axis) + 1e-06)

    down = jnp.where(free_down, ratio(on_first, by_y[:vectors], by_xp[:vectors], 1), 0.0)
    along = jnp.where(
        free_along, ratio(on_second, shifted_y[:vectors], shifted_xp[:vectors], 0), 0.0
    )

    lane = iota((width, 128), 1)
    line = iota((width, 128), 0)
    is_first = lane < vectors
    is_second = (lane >= vectors) & (lane < 2 * vectors)
    is_third = (lane >= 2 * vectors) & (lane < width)
    square = jnp.concatenate(
        [jnp.where(lane < vectors, by_y, 0.0), jnp.zeros((128 - width, 128), F32)], axis=0
    )
    y_rows = jnp.transpose(square)[:vectors]
    zero_w = jnp.zeros((vectors, 128), F32)
    over_x = jnp.concatenate([by_xp[:vectors], y_rows, by_xp[vectors:]], axis=0)
    over_x_next = jnp.concatenate(
        [shifted_xp[:vectors], pltpu.roll(y_rows, vectors, 1), shifted_xp[vectors:]], axis=0
    )
    over_p = jnp.concatenate([shifted_xp[:vectors], y_rows, shifted_xp[vectors:]], axis=0)
    gate = jnp.where(free_along, 1.0, 0.0)

    def residual_rows(values):
        first, second, third = [values[i * vectors : (i + 1) * vectors] for i in range(3)]
        return jnp.concatenate(
            [first, jnp.where(free_down, down * first - second, 0.0), third], axis=0
        )

    def three(first, second, third):
        return jnp.where(
            is_first, first, jnp.where(is_second, second, jnp.where(is_third, third, 0.0))
        )

    gram = residual_rows(
        three(over_x, over_x_next * along - shifted_y * gate, over_p)
    )
    gram = gram * scale

    rest = gram[vectors : 2 * vectors]
    frozen = on_second & (line_w < locked)
    small = jnp.where(middle_w, rest + jnp.where(frozen, 1.0, 0.0), 0.0)
    small = small + jnp.where(lane_w == line_w + 2 * vectors, 1.0, 0.0)
    padded = (line == lane) & (line >= vectors) & (line < vectors + locked)
    big = gram + jnp.where(padded | (lane == line + width), 1.0, 0.0)

    step = 4
    small_rows = []
    for k in range(0, vectors, step):
        small, done = panel(small, k, vectors, step)
        small_rows += done
    inverse_w = jnp.concatenate(small_rows, axis=0)[:, 2 * vectors : 3 * vectors]

    def outputs():
        high, low = split(inverse_w)
        lhs = jnp.concatenate(
            [jnp.concatenate([high, high], axis=1), jnp.concatenate([low, low], axis=1)], axis=0
        )

        def turn(values):
            rhs = jnp.concatenate(split(values), axis=0)
            out = jnp.dot(lhs, rhs, preferred_element_type=F32)
            return out[:vectors] + out[vectors:]

        for t in range(row_tiles):
            lanes = slice(t * tile, (t + 1) * tile)
            image = yh[reach + t]
            residual = jnp.where(free_down, down * xh[reach + t] - image, 0.0)
            carried = jnp.where(free_down, down * image - z_buf[t], 0.0)
            w_ref[:, lanes] = turn(residual)
            aw_ref[:, lanes] = turn(residual - carried)

    for k in range(0, width, step):
        if k == 2 * vectors:
            outputs()
        big, done = panel(big, k, 0, step)
        for i in range(step):
            upper[k + i : k + i + 1, :] = done[i]
    inverse = upper[:, width : 2 * width]

    by_q = unpack(all_q[1](), width, vectors, 2 * vectors)
    early = residual_rows(three(by_y, shifted_y * along, by_q))
    image = (gram - scale * early)[:, :width]
    half = jnp.dot(inverse, image, precision=HIGHEST, preferred_element_type=F32)
    first = lax.dot_general(half, inverse, NT_DIMS, precision=HIGHEST, preferred_element_type=F32)
    second = lax.dot_general(inverse, half, NT_DIMS, precision=HIGHEST, preferred_element_type=F32)
    base = first + second
    inverse_high, inverse_low = split(inverse)
    left = jnp.concatenate([inverse_high, inverse_low, inverse_high], axis=1)
    right = jnp.concatenate([inverse_high, inverse_high, inverse_low], axis=1)

    by_z = unpack(all_z[1](), width, vectors, vectors)
    late = residual_rows(by_z)[:, :width]
    late = jnp.where(is_second[:, :width], late, 0.0) * gate[:, :width]
    late_high, late_low = split(late * scale)
    half = jnp.dot(
        left,
        jnp.concatenate([late_high, late_high, late_low], axis=0),
        preferred_element_type=F32,
    )
    half_high, half_low = split(half)
    half = jnp.concatenate([half_high, half_low, half_high], axis=1)
    first = lax.dot_general(half, right, NT_DIMS, preferred_element_type=F32)
    second = lax.dot_general(right, half, NT_DIMS, preferred_element_type=F32)
    ritz_ref[...] = 0.5 * (base + (first + second))

    halo_sent(x_halo)
    halo_sent(p_halo)
    halo_sent(y_halo)
    for done in (near_x, far_x, all_y, all_q, all_z):
        done[2]()


def store_kernel(w_ref, aw_ref, ritz_ref, w_hbm, aw_hbm, ritz_hbm, sem):
    copies = [
        pltpu.make_async_copy(source, target, sem.at[i])
        for i, (source, target) in enumerate(
            ((w_ref, w_hbm), (aw_ref, aw_hbm), (ritz_ref, ritz_hbm))
        )
    ]
    for copy in copies:
        copy.start()
    for copy in copies:
        copy.wait()


def body(sizes, current_block, previous_block, adjacency_tiles, tile_rows, tile_cols, tile_count, locked):
    vectors, here = current_block.shape
    slots, tile, _ = adjacency_tiles.shape
    row_tiles = here // tile
    row_count, col_count, sub_count = sizes
    near_count = col_count * sub_count
    total = row_count * near_count
    width = 3 * vectors
    spare = slots - row_tiles
    vmem = pl.BlockSpec(memory_space=pltpu.VMEM)
    anywhere = pl.BlockSpec(memory_space=pl.ANY)
    dma = pltpu.SemaphoreType.DMA
    grid = (2 * row_tiles, vectors, tile)
    own = (row_tiles, vectors, tile)
    shapes = (
        jax.ShapeDtypeStruct((vectors, here), F32),
        jax.ShapeDtypeStruct((vectors, here), F32),
        jax.ShapeDtypeStruct((width, width), F32),
    )
    used = 2 * slots + 2
    ints = jnp.concatenate(
        [tile_cols, tile_rows, tile_count, locked, jnp.zeros((-used % 128,), jnp.int32)]
    )
    results = pl.pallas_call(
        functools.partial(iterate_kernel, sizes, here * total),
        out_shape=shapes,
        in_specs=[anywhere] * 4,
        out_specs=(vmem, vmem, vmem),
        scratch_shapes=[
            pltpu.SMEM(ints.shape, jnp.int32),
            pltpu.SMEM((spare,), jnp.int32),
            pltpu.SMEM((spare,), jnp.int32),
            pltpu.SMEM((row_tiles,), jnp.int32),
            pltpu.VMEM((slots, tile, tile), F32),
            pltpu.VMEM((slots, 2 * tile, tile), BF16),
            pltpu.VMEM(grid, F32),
            pltpu.VMEM(grid, F32),
            pltpu.VMEM(grid, F32),
            pltpu.VMEM(own, F32),
            pltpu.VMEM(own, F32),
            pltpu.VMEM((spare + 1, vectors, tile), F32),
            pltpu.VMEM((4, near_count, EDGE, 128), F32),
            pltpu.VMEM((4, row_count, EDGE, 128), F32),
            pltpu.VMEM((3, total, EDGE, 128), F32),
            pltpu.VMEM((width, 128), F32),
            dma((1,)),
            dma((2,)),
            dma((slots // row_tiles,)),
            dma((3, 2)),
            dma((3, 2)),
            dma((4,)),
            dma((4,)),
            dma((4,)),
            dma((4,)),
            dma((3,)),
            dma((3,)),
            pltpu.SemaphoreType.REGULAR((2,)),
        ],
        compiler_params=pltpu.CompilerParams(
            collective_id=0, has_side_effects=True, vmem_limit_bytes=VMEM_ALL - VMEM_ROOM
        ),
        name="iterate",
    )(ints, current_block, previous_block, adjacency_tiles)
    return pl.pallas_call(
        store_kernel,
        out_shape=shapes,
        in_specs=[vmem] * 3,
        out_specs=(anywhere,) * 3,
        scratch_shapes=[dma((3,))],
        compiler_params=pltpu.CompilerParams(vmem_limit_bytes=VMEM_ALL - VMEM_ROOM),
        name="store",
    )(*results)


def solution(mesh):
    split_all = ("graphs", "rows", "cols", "sub")
    sizes = tuple(mesh.shape[name] for name in ("rows", "cols", "sub"))
    in_specs = (
        P(None, split_all),
        P(None, split_all),
        P(split_all, None, None),
        P(split_all),
        P(split_all),
        P(split_all),
        P("graphs"),
    )
    out_specs = (P(None, split_all), P(None, split_all), P("graphs", None))
    return jax.shard_map(
        functools.partial(body, sizes), mesh=mesh, in_specs=in_specs, out_specs=out_specs, check_vma=False
    )
```

```python
import functools

import jax
import jax.numpy as jnp
from jax import lax
from jax.experimental import pallas as pl
from jax.experimental.pallas import tpu as pltpu
from jax.sharding import PartitionSpec as P

MESH = pl.DeviceIdType.MESH
F32 = jnp.float32
BF16 = jnp.bfloat16
HIGHEST = lax.Precision.HIGHEST
NT_DIMS = (((1,), (1,)), ((), ()))
EDGE = 8
VMEM_ALL = 67043328
VMEM_ROOM = 10600 * 1024


def split(values):
    high = values.astype(BF16)
    return high, (values - high.astype(F32)).astype(BF16)


def iota(shape, dim):
    return lax.broadcasted_iota(jnp.int32, shape, dim)


def tree_sum(terms):
    while len(terms) > 1:
        terms = [a + b for a, b in zip(terms[::2], terms[1::2])] + terms[len(terms) & ~1 :]
    return terms[0]


def panel(matrix, k, shift, count):
    rows = [matrix[k + i : k + i + 1, :] for i in range(count)]
    columns = [
        jnp.broadcast_to(matrix[:, shift + k + i : shift + k + i + 1], matrix.shape)
        for i in range(count)
    ]
    block = {
        (i, j): jnp.broadcast_to(rows[i][:, shift + k + j : shift + k + j + 1], (1, 128))
        for i in range(count)
        for j in range(i, count)
    }
    done = []
    for m in range(count):
        inverse = 1.0 / block[m, m]
        done.append(rows[m] * lax.rsqrt(block[m, m]))
        factors = {j: block[m, j] * inverse for j in range(m + 1, count)}
        for i in range(m + 1, count):
            for j in range(i, count):
                block[i, j] = block[i, j] - factors[i] * block[m, j]
            rows[i] = rows[i] - factors[i] * rows[m]
            columns[i] = columns[i] - factors[i] * columns[m]
        matrix = matrix - columns[m] * (rows[m] * inverse)
    return matrix, done


def iterate_kernel(
    sizes, vertex_total,
    cols_in, rows_in, count_in, locked_in, x_hbm, p_hbm, tiles_hbm,
    w_ref, aw_ref, ritz_ref,
    cols_ref, rows_ref, count_ref, locked_ref, index_ref, before_ref, last_ref,
    raw, halves, xh, ph, yh, q_buf, z_buf, seg, near_ref, far_ref, every, upper,
    int_sem, block_sem, tile_sem, halo_send, halo_recv, near_send, near_recv, far_send, far_recv,
    all_send, all_recv, relay,
):
    row_count, col_count, sub_count = sizes
    near_count = col_count * sub_count
    total = row_count * near_count
    vectors, here = w_ref.shape
    slots, tile, _ = raw.shape
    row_tiles = here // tile
    reach = row_tiles // 2
    spare = slots - row_tiles
    chunk = row_tiles
    chunks = slots // chunk
    width = 3 * vectors

    row_at = lax.axis_index("rows")
    col_at = lax.axis_index("cols")
    sub_at = lax.axis_index("sub")
    position = row_at * near_count + col_at * sub_count + sub_at

    def place(spot):
        return {
            "rows": lax.div(spot, near_count),
            "cols": lax.div(lax.rem(spot, near_count), sub_count),
            "sub": lax.rem(spot, sub_count),
        }

    rows_from = [lax.rem(row_at + k, row_count) for k in range(row_count)]
    cols_from = [lax.rem(col_at + k, col_count) for k in range(col_count)]
    subs_from = [lax.rem(sub_at + k, sub_count) for k in range(sub_count)]

    has_left = position > 0
    has_right = position < total - 1
    has_under = row_at > 0
    has_over = row_at < row_count - 1
    left_device = place(lax.max(position - 1, 0))
    right_device = place(lax.min(position + 1, total - 1))
    under_device = {"rows": lax.max(row_at - 1, 0)}
    over_device = {"rows": lax.min(row_at + 1, row_count - 1)}
    near_at = col_at * sub_count + sub_at
    crosses_left = has_left & (near_at == 0)
    crosses_right = has_right & (near_at == near_count - 1)

    def near_device(k):
        return {"cols": cols_from[k // sub_count], "sub": subs_from[k % sub_count]}

    def far_device(k):
        return {"rows": rows_from[k]}

    def any_device(k):
        turn = (k - 1) // near_count
        if turn == row_count - 1:
            return near_device(k - turn * near_count)
        up = turn + jnp.where(turn >= row_at, 1, 0)
        down = row_count - 1 - turn
        down = down - jnp.where(down <= row_at, 1, 0)
        return {"rows": jnp.where(2 * row_at >= row_count, up, down)} | near_device((k - 1) % near_count)

    def signal(semaphore, device):
        pl.semaphore_signal(semaphore, inc=1, device_id=device, device_id_type=MESH)

    barrier = pltpu.get_barrier_semaphore()
    greeted = near_count - 1
    for there, device in (
        (crosses_left, left_device),
        (crosses_right, right_device),
        (has_under, under_device),
        (has_over, over_device),
    ):
        pl.when(there)(functools.partial(signal, barrier, device))
        greeted = greeted + jnp.where(there, 1, 0)
    for k in range(1, near_count):
        signal(barrier, near_device(k))

    def tell():
        pl.when(has_under)(functools.partial(signal, relay.at[1], under_device))
        pl.when(has_over)(functools.partial(signal, relay.at[0], over_device))

    def hear():
        pl.when(has_under)(lambda: pl.semaphore_wait(relay.at[0], 1))
        pl.when(has_over)(lambda: pl.semaphore_wait(relay.at[1], 1))

    def hear_rest():
        hear()

        def step(k, carry):
            tell()
            hear()
            return carry

        if row_count > 4:
            lax.fori_loop(0, row_count - 4, step, 0)

    own = pl.ds(reach, row_tiles)

    def block_start(source, target, sem):
        for t in range(row_tiles):
            pltpu.make_async_copy(
                source.at[:, pl.ds(t * tile, tile)], target.at[reach + t], sem
            ).start()

    def block_wait(target, sem):
        pltpu.make_async_copy(target.at[own], target.at[own], sem).wait()

    block_start(x_hbm, xh, block_sem.at[0])
    int_copies = [
        pltpu.make_async_copy(source, target, int_sem.at[i])
        for i, (source, target) in enumerate(
            (
                (cols_in, cols_ref),
                (rows_in, rows_ref),
                (count_in, count_ref),
                (locked_in, locked_ref),
            )
        )
    ]
    for copy in int_copies:
        copy.start()
    tile_copies = []
    for c in range(chunks):
        part = pl.ds(c * chunk, chunk)
        tile_copies.append(pltpu.make_async_copy(tiles_hbm.at[part], raw.at[part], tile_sem.at[c]))
    tile_copies[0].start()
    block_start(p_hbm, ph, block_sem.at[1])
    for copy in tile_copies[1:]:
        copy.start()

    def halo_copies(buffer, which):
        left = pltpu.make_async_remote_copy(
            src_ref=buffer.at[pl.ds(reach, reach)],
            dst_ref=buffer.at[pl.ds(reach + row_tiles, reach)],
            send_sem=halo_send.at[which, 0],
            recv_sem=halo_recv.at[which, 0],
            device_id=left_device,
            device_id_type=MESH,
        )
        right = pltpu.make_async_remote_copy(
            src_ref=buffer.at[pl.ds(row_tiles, reach)],
            dst_ref=buffer.at[pl.ds(0, reach)],
            send_sem=halo_send.at[which, 1],
            recv_sem=halo_recv.at[which, 1],
            device_id=right_device,
            device_id_type=MESH,
        )
        return left, right

    def halo_do(first_when, first, second_when, second):
        @pl.when(first_when)
        def _():
            first()

        @pl.when(second_when)
        def _():
            second()

    def halo_start(copies):
        halo_do(has_left, copies[0].start, has_right, copies[1].start)

    def halo_arrived(copies):
        halo_do(has_right, copies[0].wait_recv, has_left, copies[1].wait_recv)

    def halo_sent(copies):
        halo_do(has_left, copies[0].wait_send, has_right, copies[1].wait_send)

    x_halo = halo_copies(xh, 0)
    p_halo = halo_copies(ph, 1)
    y_halo = halo_copies(yh, 2)

    block_wait(xh, block_sem.at[0])
    pl.semaphore_wait(barrier, greeted)
    halo_start(x_halo)
    tell()

    def product(block, slot):
        high, low = split(block)
        lhs = jnp.concatenate(
            [jnp.concatenate([high, high], axis=1), jnp.concatenate([low, low], axis=1)], axis=0
        )
        out = jnp.dot(lhs, halves[slot], preferred_element_type=F32)
        return out[:vectors] + out[vectors:]

    def split_tiles(c):
        tile_copies[c].wait()

        def step(i, carry):
            for j in range(2):
                t = c * chunk + 2 * i + j
                high, low = split(raw[t])
                halves[t, 0:tile, :] = high
                halves[t, tile : 2 * tile, :] = low
            return carry

        lax.fori_loop(0, chunk // 2, step, 0)

    def diagonal(source, target, target_base):
        def step(g, carry):
            for i in range(8):
                r = g * 8 + i
                target[target_base + r] = product(source[reach + r], r)
            return carry

        lax.fori_loop(0, row_tiles // 8, step, 0)

    def tables():
        for copy in int_copies:
            copy.wait()
        live = count_ref[0]
        base_col = position * row_tiles - reach
        base_row = position * row_tiles
        at = []
        for t in range(spare):
            index_ref[t] = jnp.clip(cols_ref[row_tiles + t] - base_col, 0, 2 * row_tiles - 1)
            row = jnp.where(row_tiles + t < live, rows_ref[row_tiles + t] - base_row, -1)
            link = jnp.int32(0)
            for s in range(t):
                link = jnp.where(at[s] == row, s + 1, link)
            before_ref[t] = link
            at.append(row)
        for r in range(row_tiles):
            link = jnp.int32(0)
            for s in range(spare):
                link = jnp.where(at[s] == r, s + 1, link)
            last_ref[r] = link

    def scattered(padded, target, target_base):
        for t in range(spare):
            out = product(padded[index_ref[t]], row_tiles + t)
            seg[t + 1] = out + seg[before_ref[t]]
        for r in range(row_tiles):
            target[target_base + r] = target[target_base + r] + seg[last_ref[r]]

    def parts(buffer, start):
        pieces = [split(buffer[start + t]) for t in range(row_tiles)]
        return [jnp.concatenate([piece[half] for piece in pieces], axis=1) for half in range(2)]

    def inner(left, right):
        lhs = jnp.concatenate([v[0] for v in left] + [v[1] for v in left], axis=0)
        rhs = jnp.concatenate([v[0] for v in right] + [v[1] for v in right], axis=0)
        half = here // 2
        out = [
            lax.dot_general(lhs[:, part], rhs[:, part], NT_DIMS, preferred_element_type=F32)
            for part in (slice(0, half), slice(half, here))
        ]
        count = len(left) * vectors
        return (out[0][:count] + out[1][:count]) + (out[0][count:] + out[1][count:])

    edge_lane = iota((EDGE, 128), 1)

    def pack(values, lanes):
        rows = values.shape[0]
        padded = jnp.concatenate([values, jnp.zeros((rows, 128 - 2 * lanes), F32)], axis=1)
        pieces = []
        for k in range(rows // EDGE):
            piece = padded[k * EDGE : (k + 1) * EDGE]
            first = piece if k == 0 else pltpu.roll(piece, k * lanes, 1)
            second = pltpu.roll(piece, (k * lanes - lanes) % 128, 1)
            here_lane = (edge_lane >= k * lanes) & (edge_lane < (k + 1) * lanes)
            pieces.append(jnp.where(here_lane, first + second, 0.0))
        return tree_sum(pieces)

    def unpack(values, rows, lanes, at=0):
        pieces = [
            values if k * lanes == at else pltpu.roll(values, (at - k * lanes) % 128, 1)
            for k in range(rows // EDGE)
        ]
        return jnp.concatenate(pieces, axis=0)

    def stage(buffer, which, height, count, at, device, send, recv):
        def start(*values):
            mine = buffer.at[which, at, pl.ds(0, height)]
            for k, value in enumerate(values):
                buffer[which, at, k * EDGE : (k + 1) * EDGE] = value
            for k in range(1, count):
                pltpu.make_async_remote_copy(
                    src_ref=mine,
                    dst_ref=mine,
                    send_sem=send.at[which],
                    recv_sem=recv.at[which],
                    device_id=device(k),
                    device_id_type=MESH,
                ).start()

        def wait(sem):
            rest = buffer.at[which, pl.ds(0, count - 1), pl.ds(0, height)]
            pltpu.make_async_copy(rest, rest, sem.at[which]).wait()

        def collect():
            wait(recv)
            return tree_sum([buffer[which, k, 0:height] for k in range(count)])

        return start, collect, lambda: wait(send)

    def near_stage(which):
        return stage(near_ref, which, EDGE, near_count, near_at, near_device, near_send, near_recv)

    def far_stage(which):
        return stage(far_ref, which, EDGE, row_count, row_at, far_device, far_send, far_recv)

    def all_stage(which):
        if total <= 32:
            return stage(every, which, EDGE, total, position, any_device, all_send, all_recv)
        first, second = near_stage(which + 1), far_stage(which + 1)

        def start(values):
            first[0](values)
            second[0](first[1]())

        def sent():
            first[2]()
            second[2]()

        return start, second[1], sent

    near_x, far_x = near_stage(0), far_stage(0)
    all_y, all_q, all_z = all_stage(0), all_stage(1), all_stage(2)

    tables()
    hear()
    tell()
    block_wait(ph, block_sem.at[1])
    seg[0] = jnp.zeros((vectors, tile), F32)
    for c in range(chunks):
        split_tiles(c)
        if c == row_tiles // chunk - 1:
            diagonal(xh, yh, reach)
    hear()
    tell()
    halo_start(p_halo)
    diagonal(ph, q_buf, 0)
    x_parts, p_parts = parts(xh, reach), parts(ph, reach)
    near_x[0](pack(inner((x_parts, p_parts), (x_parts, p_parts)), 2 * vectors))

    hear_rest()
    halo_arrived(x_halo)
    scattered(xh, yh, reach)
    halo_start(y_halo)
    y_parts = parts(yh, reach)
    basis = (x_parts, y_parts, p_parts)
    all_y[0](pack(inner(basis, (y_parts,)), vectors))

    far_x[0](near_x[1]())
    halo_arrived(p_halo)
    scattered(ph, q_buf, 0)
    all_q[0](pack(inner(basis, (parts(q_buf, 0),)), vectors))
    diagonal(yh, z_buf, 0)
    halo_arrived(y_halo)
    scattered(yh, z_buf, 0)
    all_z[0](pack(inner(basis, (parts(z_buf, 0),)), vectors))

    scale = 1.0 / vertex_total
    locked = locked_ref[0]
    by_xp = unpack(far_x[1](), 2 * vectors, 2 * vectors)
    by_y = unpack(all_y[1](), width, vectors)
    lane_w = iota((vectors, 128), 1)
    line_w = iota((vectors, 128), 0)
    middle_w = (lane_w >= vectors) & (lane_w < 2 * vectors)
    shifted_y = pltpu.roll(by_y, vectors, 1)
    shifted_xp = pltpu.roll(by_xp, vectors, 1)
    on_first = lane_w == line_w
    on_second = lane_w == line_w + vectors
    free_down = iota((vectors, 1), 0) >= locked
    free_along = (iota((1, 128), 1) >= vectors + locked) & (iota((1, 128), 1) < 2 * vectors)

    def diagonal_of(mask, values, axis):
        return jnp.sum(jnp.where(mask, values, 0.0), axis=axis, keepdims=True)

    def ratio(mask, over, under, axis):
        return (diagonal_of(mask, over, axis) + 1e-06) / (diagonal_of(mask, under, axis) + 1e-06)

    down = jnp.where(free_down, ratio(on_first, by_y[:vectors], by_xp[:vectors], 1), 0.0)
    along = jnp.where(
        free_along, ratio(on_second, shifted_y[:vectors], shifted_xp[:vectors], 0), 0.0
    )

    lane = iota((width, 128), 1)
    line = iota((width, 128), 0)
    is_first = lane < vectors
    is_second = (lane >= vectors) & (lane < 2 * vectors)
    is_third = (lane >= 2 * vectors) & (lane < width)
    square = jnp.concatenate(
        [jnp.where(lane < vectors, by_y, 0.0), jnp.zeros((128 - width, 128), F32)], axis=0
    )
    y_rows = jnp.transpose(square)[:vectors]
    zero_w = jnp.zeros((vectors, 128), F32)
    over_x = jnp.concatenate([by_xp[:vectors], y_rows, by_xp[vectors:]], axis=0)
    over_x_next = jnp.concatenate(
        [shifted_xp[:vectors], pltpu.roll(y_rows, vectors, 1), shifted_xp[vectors:]], axis=0
    )
    over_p = jnp.concatenate([shifted_xp[:vectors], y_rows, shifted_xp[vectors:]], axis=0)
    gate = jnp.where(free_along, 1.0, 0.0)

    def residual_rows(values):
        first, second, third = [values[i * vectors : (i + 1) * vectors] for i in range(3)]
        return jnp.concatenate(
            [first, jnp.where(free_down, down * first - second, 0.0), third], axis=0
        )

    def three(first, second, third):
        return jnp.where(
            is_first, first, jnp.where(is_second, second, jnp.where(is_third, third, 0.0))
        )

    gram = residual_rows(
        three(over_x, over_x_next * along - shifted_y * gate, over_p)
    )
    gram = gram * scale

    rest = gram[vectors : 2 * vectors]
    frozen = on_second & (line_w < locked)
    small = jnp.where(middle_w, rest + jnp.where(frozen, 1.0, 0.0), 0.0)
    small = small + jnp.where(lane_w == line_w + 2 * vectors, 1.0, 0.0)
    padded = (line == lane) & (line >= vectors) & (line < vectors + locked)
    big = gram + jnp.where(padded | (lane == line + width), 1.0, 0.0)

    step = 4
    small_rows = []
    for k in range(0, vectors, step):
        small, done = panel(small, k, vectors, step)
        small_rows += done
    inverse_w = jnp.concatenate(small_rows, axis=0)[:, 2 * vectors : 3 * vectors]

    def outputs():
        high, low = split(inverse_w)
        lhs = jnp.concatenate(
            [jnp.concatenate([high, high], axis=1), jnp.concatenate([low, low], axis=1)], axis=0
        )

        def turn(values):
            rhs = jnp.concatenate(split(values), axis=0)
            out = jnp.dot(lhs, rhs, preferred_element_type=F32)
            return out[:vectors] + out[vectors:]

        for t in range(row_tiles):
            lanes = slice(t * tile, (t + 1) * tile)
            image = yh[reach + t]
            residual = jnp.where(free_down, down * xh[reach + t] - image, 0.0)
            carried = jnp.where(free_down, down * image - z_buf[t], 0.0)
            w_ref[:, lanes] = turn(residual)
            aw_ref[:, lanes] = turn(residual - carried)

    for k in range(0, width, step):
        if k == 2 * vectors:
            outputs()
        big, done = panel(big, k, 0, step)
        for i in range(step):
            upper[k + i : k + i + 1, :] = done[i]
    inverse = upper[:, width : 2 * width]

    by_q = unpack(all_q[1](), width, vectors, 2 * vectors)
    early = residual_rows(three(by_y, shifted_y * along, by_q))
    image = (gram - scale * early)[:, :width]
    half = jnp.dot(inverse, image, precision=HIGHEST, preferred_element_type=F32)
    first = lax.dot_general(half, inverse, NT_DIMS, precision=HIGHEST, preferred_element_type=F32)
    second = lax.dot_general(inverse, half, NT_DIMS, precision=HIGHEST, preferred_element_type=F32)
    base = first + second
    inverse_high, inverse_low = split(inverse)
    left = jnp.concatenate([inverse_high, inverse_low, inverse_high], axis=1)
    right = jnp.concatenate([inverse_high, inverse_high, inverse_low], axis=1)

    by_z = unpack(all_z[1](), width, vectors, vectors)
    late = residual_rows(by_z)[:, :width]
    late = jnp.where(is_second[:, :width], late, 0.0) * gate[:, :width]
    late_high, late_low = split(late * scale)
    half = jnp.dot(
        left,
        jnp.concatenate([late_high, late_high, late_low], axis=0),
        preferred_element_type=F32,
    )
    half_high, half_low = split(half)
    half = jnp.concatenate([half_high, half_low, half_high], axis=1)
    first = lax.dot_general(half, right, NT_DIMS, preferred_element_type=F32)
    second = lax.dot_general(right, half, NT_DIMS, preferred_element_type=F32)
    ritz_ref[...] = 0.5 * (base + (first + second))

    halo_sent(x_halo)
    halo_sent(p_halo)
    halo_sent(y_halo)
    for done in (near_x, far_x, all_y, all_q, all_z):
        done[2]()


def store_kernel(w_ref, aw_ref, ritz_ref, w_hbm, aw_hbm, ritz_hbm, sem):
    copies = [
        pltpu.make_async_copy(source, target, sem.at[i])
        for i, (source, target) in enumerate(
            ((w_ref, w_hbm), (aw_ref, aw_hbm), (ritz_ref, ritz_hbm))
        )
    ]
    for copy in copies:
        copy.start()
    for copy in copies:
        copy.wait()


def body(sizes, current_block, previous_block, adjacency_tiles, tile_rows, tile_cols, tile_count, locked):
    vectors, here = current_block.shape
    slots, tile, _ = adjacency_tiles.shape
    row_tiles = here // tile
    row_count, col_count, sub_count = sizes
    near_count = col_count * sub_count
    total = row_count * near_count
    width = 3 * vectors
    spare = slots - row_tiles
    vmem = pl.BlockSpec(memory_space=pltpu.VMEM)
    anywhere = pl.BlockSpec(memory_space=pl.ANY)
    dma = pltpu.SemaphoreType.DMA
    grid = (2 * row_tiles, vectors, tile)
    own = (row_tiles, vectors, tile)
    shapes = (
        jax.ShapeDtypeStruct((vectors, here), F32),
        jax.ShapeDtypeStruct((vectors, here), F32),
        jax.ShapeDtypeStruct((width, width), F32),
    )
    iterate = pl.pallas_call(
        functools.partial(iterate_kernel, sizes, here * total),
        out_shape=shapes,
        in_specs=[anywhere] * 7,
        out_specs=(vmem, vmem, vmem),
        scratch_shapes=[
            pltpu.SMEM((slots,), jnp.int32),
            pltpu.SMEM((slots,), jnp.int32),
            pltpu.SMEM((1,), jnp.int32),
            pltpu.SMEM((1,), jnp.int32),
            pltpu.SMEM((spare,), jnp.int32),
            pltpu.SMEM((spare,), jnp.int32),
            pltpu.SMEM((row_tiles,), jnp.int32),
            pltpu.VMEM((slots, tile, tile), F32),
            pltpu.VMEM((slots, 2 * tile, tile), BF16),
            pltpu.VMEM(grid, F32),
            pltpu.VMEM(grid, F32),
            pltpu.VMEM(grid, F32),
            pltpu.VMEM(own, F32),
            pltpu.VMEM(own, F32),
            pltpu.VMEM((spare + 1, vectors, tile), F32),
            pltpu.VMEM((4, near_count, EDGE, 128), F32),
            pltpu.VMEM((4, row_count, EDGE, 128), F32),
            pltpu.VMEM((3, total, EDGE, 128), F32),
            pltpu.VMEM((width, 128), F32),
            dma((4,)),
            dma((2,)),
            dma((slots // row_tiles,)),
            dma((3, 2)),
            dma((3, 2)),
            dma((4,)),
            dma((4,)),
            dma((4,)),
            dma((4,)),
            dma((3,)),
            dma((3,)),
            pltpu.SemaphoreType.REGULAR((2,)),
        ],
        compiler_params=pltpu.CompilerParams(
            collective_id=0, has_side_effects=True, vmem_limit_bytes=VMEM_ALL - VMEM_ROOM
        ),
        name="iterate",
    )
    results = lax.cond(
        lax.axis_index("rows") >= 0,
        iterate,
        lambda *_: tuple(jnp.zeros(shape.shape, F32) for shape in shapes),
        tile_cols, tile_rows, tile_count, locked, current_block, previous_block, adjacency_tiles,
    )
    return pl.pallas_call(
        store_kernel,
        out_shape=shapes,
        in_specs=[vmem] * 3,
        out_specs=(anywhere,) * 3,
        scratch_shapes=[dma((3,))],
        compiler_params=pltpu.CompilerParams(vmem_limit_bytes=VMEM_ALL - VMEM_ROOM),
        name="store",
    )(*results)


def solution(mesh):
    split_all = ("graphs", "rows", "cols", "sub")
    sizes = tuple(mesh.shape[name] for name in ("rows", "cols", "sub"))
    in_specs = (
        P(None, split_all),
        P(None, split_all),
        P(split_all, None, None),
        P(split_all),
        P(split_all),
        P(split_all),
        P("graphs"),
    )
    out_specs = (P(None, split_all), P(None, split_all), P("graphs", None))
    return jax.shard_map(
        functools.partial(body, sizes), mesh=mesh, in_specs=in_specs, out_specs=out_specs, check_vma=False
    )
```

```python
import functools

import jax
import jax.numpy as jnp
from jax import lax
from jax.experimental import pallas as pl
from jax.experimental.pallas import tpu as pltpu
from jax.sharding import PartitionSpec as P

MESH = pl.DeviceIdType.MESH
F32 = jnp.float32
BF16 = jnp.bfloat16
HIGHEST = lax.Precision.HIGHEST
NT_DIMS = (((1,), (1,)), ((), ()))
EDGE = 8
VMEM_ALL = 67043328
VMEM_ROOM = 10600 * 1024


def split(values):
    high = values.astype(BF16)
    return high, (values - high.astype(F32)).astype(BF16)


def iota(shape, dim):
    return lax.broadcasted_iota(jnp.int32, shape, dim)


def tree_sum(terms):
    while len(terms) > 1:
        terms = [a + b for a, b in zip(terms[::2], terms[1::2])] + terms[len(terms) & ~1 :]
    return terms[0]


def panel(matrix, k, shift, count):
    rows = [matrix[k + i : k + i + 1, :] for i in range(count)]
    columns = [
        jnp.broadcast_to(matrix[:, shift + k + i : shift + k + i + 1], matrix.shape)
        for i in range(count)
    ]
    block = {
        (i, j): jnp.broadcast_to(rows[i][:, shift + k + j : shift + k + j + 1], (1, 128))
        for i in range(count)
        for j in range(i, count)
    }
    done = []
    for m in range(count):
        inverse = 1.0 / block[m, m]
        done.append(rows[m] * lax.rsqrt(block[m, m]))
        factors = {j: block[m, j] * inverse for j in range(m + 1, count)}
        for i in range(m + 1, count):
            for j in range(i, count):
                block[i, j] = block[i, j] - factors[i] * block[m, j]
            rows[i] = rows[i] - factors[i] * rows[m]
            columns[i] = columns[i] - factors[i] * columns[m]
        matrix = matrix - columns[m] * (rows[m] * inverse)
    return matrix, done


def iterate_kernel(
    sizes, vertex_total,
    cols_in, rows_in, count_in, locked_in, x_hbm, p_hbm, tiles_hbm,
    w_ref, aw_ref, ritz_ref,
    cols_ref, rows_ref, count_ref, locked_ref, index_ref, before_ref, last_ref,
    raw, halves, xh, ph, yh, q_buf, z_buf, seg, near_ref, far_ref, every, upper,
    int_sem, block_sem, tile_sem, halo_send, halo_recv, near_send, near_recv, far_send, far_recv,
    all_send, all_recv, relay,
):
    row_count, col_count, sub_count = sizes
    near_count = col_count * sub_count
    total = row_count * near_count
    vectors, here = w_ref.shape
    slots, tile, _ = raw.shape
    row_tiles = here // tile
    reach = row_tiles // 2
    spare = slots - row_tiles
    chunk = row_tiles
    chunks = slots // chunk
    width = 3 * vectors

    row_at = lax.axis_index("rows")
    col_at = lax.axis_index("cols")
    sub_at = lax.axis_index("sub")
    position = row_at * near_count + col_at * sub_count + sub_at

    def place(spot):
        return {
            "rows": lax.div(spot, near_count),
            "cols": lax.div(lax.rem(spot, near_count), sub_count),
            "sub": lax.rem(spot, sub_count),
        }

    rows_from = [lax.rem(row_at + k, row_count) for k in range(row_count)]
    cols_from = [lax.rem(col_at + k, col_count) for k in range(col_count)]
    subs_from = [lax.rem(sub_at + k, sub_count) for k in range(sub_count)]

    has_left = position > 0
    has_right = position < total - 1
    has_under = row_at > 0
    has_over = row_at < row_count - 1
    left_device = place(lax.max(position - 1, 0))
    right_device = place(lax.min(position + 1, total - 1))
    under_device = {"rows": lax.max(row_at - 1, 0)}
    over_device = {"rows": lax.min(row_at + 1, row_count - 1)}
    near_at = col_at * sub_count + sub_at
    crosses_left = has_left & (near_at == 0)
    crosses_right = has_right & (near_at == near_count - 1)

    def near_device(k):
        return {"cols": cols_from[k // sub_count], "sub": subs_from[k % sub_count]}

    def far_device(k):
        return {"rows": rows_from[k]}

    def any_device(k):
        turn = (k - 1) // near_count
        if turn == row_count - 1:
            return near_device(k - turn * near_count)
        up = turn + jnp.where(turn >= row_at, 1, 0)
        down = row_count - 1 - turn
        down = down - jnp.where(down <= row_at, 1, 0)
        return {"rows": jnp.where(2 * row_at >= row_count, up, down)} | near_device((k - 1) % near_count)

    def signal(semaphore, device):
        pl.semaphore_signal(semaphore, inc=1, device_id=device, device_id_type=MESH)

    barrier = pltpu.get_barrier_semaphore()
    greeted = near_count - 1
    for there, device in (
        (crosses_left, left_device),
        (crosses_right, right_device),
        (has_under, under_device),
        (has_over, over_device),
    ):
        pl.when(there)(functools.partial(signal, barrier, device))
        greeted = greeted + jnp.where(there, 1, 0)
    for k in range(1, near_count):
        signal(barrier, near_device(k))

    def tell():
        pl.when(has_under)(functools.partial(signal, relay.at[1], under_device))
        pl.when(has_over)(functools.partial(signal, relay.at[0], over_device))

    def hear():
        pl.when(has_under)(lambda: pl.semaphore_wait(relay.at[0], 1))
        pl.when(has_over)(lambda: pl.semaphore_wait(relay.at[1], 1))

    def hear_rest():
        hear()

        def step(k, carry):
            tell()
            hear()
            return carry

        if row_count > 4:
            lax.fori_loop(0, row_count - 4, step, 0)

    own = pl.ds(reach, row_tiles)

    def block_start(source, target, sem):
        for t in range(row_tiles):
            pltpu.make_async_copy(
                source.at[:, pl.ds(t * tile, tile)], target.at[reach + t], sem
            ).start()

    def block_wait(target, sem):
        pltpu.make_async_copy(target.at[own], target.at[own], sem).wait()

    block_start(x_hbm, xh, block_sem.at[0])
    int_copies = [
        pltpu.make_async_copy(source, target, int_sem.at[i])
        for i, (source, target) in enumerate(
            (
                (cols_in, cols_ref),
                (rows_in, rows_ref),
                (count_in, count_ref),
                (locked_in, locked_ref),
            )
        )
    ]
    tile_copies = []
    for c in range(chunks):
        part = pl.ds(c * chunk, chunk)
        tile_copies.append(pltpu.make_async_copy(tiles_hbm.at[part], raw.at[part], tile_sem.at[c]))
    tile_copies[0].start()
    block_start(p_hbm, ph, block_sem.at[1])
    for copy in tile_copies[1:]:
        copy.start()
    for copy in int_copies:
        copy.start()

    def halo_copies(buffer, which):
        left = pltpu.make_async_remote_copy(
            src_ref=buffer.at[pl.ds(reach, reach)],
            dst_ref=buffer.at[pl.ds(reach + row_tiles, reach)],
            send_sem=halo_send.at[which, 0],
            recv_sem=halo_recv.at[which, 0],
            device_id=left_device,
            device_id_type=MESH,
        )
        right = pltpu.make_async_remote_copy(
            src_ref=buffer.at[pl.ds(row_tiles, reach)],
            dst_ref=buffer.at[pl.ds(0, reach)],
            send_sem=halo_send.at[which, 1],
            recv_sem=halo_recv.at[which, 1],
            device_id=right_device,
            device_id_type=MESH,
        )
        return left, right

    def halo_do(first_when, first, second_when, second):
        @pl.when(first_when)
        def _():
            first()

        @pl.when(second_when)
        def _():
            second()

    def halo_start(copies):
        halo_do(has_left, copies[0].start, has_right, copies[1].start)

    def halo_arrived(copies):
        halo_do(has_right, copies[0].wait_recv, has_left, copies[1].wait_recv)

    def halo_sent(copies):
        halo_do(has_left, copies[0].wait_send, has_right, copies[1].wait_send)

    x_halo = halo_copies(xh, 0)
    p_halo = halo_copies(ph, 1)
    y_halo = halo_copies(yh, 2)

    block_wait(xh, block_sem.at[0])
    pl.semaphore_wait(barrier, greeted)
    halo_start(x_halo)
    tell()

    def product(block, slot):
        high, low = split(block)
        lhs = jnp.concatenate(
            [jnp.concatenate([high, high], axis=1), jnp.concatenate([low, low], axis=1)], axis=0
        )
        out = jnp.dot(lhs, halves[slot], preferred_element_type=F32)
        return out[:vectors] + out[vectors:]

    def split_tiles(c):
        tile_copies[c].wait()

        def step(i, carry):
            for j in range(2):
                t = c * chunk + 2 * i + j
                high, low = split(raw[t])
                halves[t, 0:tile, :] = high
                halves[t, tile : 2 * tile, :] = low
            return carry

        lax.fori_loop(0, chunk // 2, step, 0)

    def diagonal(source, target, target_base):
        def step(g, carry):
            for i in range(8):
                r = g * 8 + i
                target[target_base + r] = product(source[reach + r], r)
            return carry

        lax.fori_loop(0, row_tiles // 8, step, 0)

    def tables():
        for copy in int_copies:
            copy.wait()
        live = count_ref[0]
        base_col = position * row_tiles - reach
        base_row = position * row_tiles
        at = []
        for t in range(spare):
            index_ref[t] = jnp.clip(cols_ref[row_tiles + t] - base_col, 0, 2 * row_tiles - 1)
            row = jnp.where(row_tiles + t < live, rows_ref[row_tiles + t] - base_row, -1)
            link = jnp.int32(0)
            for s in range(t):
                link = jnp.where(at[s] == row, s + 1, link)
            before_ref[t] = link
            at.append(row)
        for r in range(row_tiles):
            link = jnp.int32(0)
            for s in range(spare):
                link = jnp.where(at[s] == r, s + 1, link)
            last_ref[r] = link

    def scattered(padded, target, target_base):
        for t in range(spare):
            out = product(padded[index_ref[t]], row_tiles + t)
            seg[t + 1] = out + seg[before_ref[t]]
        for r in range(row_tiles):
            target[target_base + r] = target[target_base + r] + seg[last_ref[r]]

    def parts(buffer, start):
        pieces = [split(buffer[start + t]) for t in range(row_tiles)]
        return [jnp.concatenate([piece[half] for piece in pieces], axis=1) for half in range(2)]

    def inner(left, right):
        lhs = jnp.concatenate([v[0] for v in left] + [v[1] for v in left], axis=0)
        rhs = jnp.concatenate([v[0] for v in right] + [v[1] for v in right], axis=0)
        half = here // 2
        out = [
            lax.dot_general(lhs[:, part], rhs[:, part], NT_DIMS, preferred_element_type=F32)
            for part in (slice(0, half), slice(half, here))
        ]
        count = len(left) * vectors
        return (out[0][:count] + out[1][:count]) + (out[0][count:] + out[1][count:])

    edge_lane = iota((EDGE, 128), 1)

    def pack(values, lanes):
        rows = values.shape[0]
        padded = jnp.concatenate([values, jnp.zeros((rows, 128 - 2 * lanes), F32)], axis=1)
        pieces = []
        for k in range(rows // EDGE):
            piece = padded[k * EDGE : (k + 1) * EDGE]
            first = piece if k == 0 else pltpu.roll(piece, k * lanes, 1)
            second = pltpu.roll(piece, (k * lanes - lanes) % 128, 1)
            here_lane = (edge_lane >= k * lanes) & (edge_lane < (k + 1) * lanes)
            pieces.append(jnp.where(here_lane, first + second, 0.0))
        return tree_sum(pieces)

    def unpack(values, rows, lanes, at=0):
        pieces = [
            values if k * lanes == at else pltpu.roll(values, (at - k * lanes) % 128, 1)
            for k in range(rows // EDGE)
        ]
        return jnp.concatenate(pieces, axis=0)

    def stage(buffer, which, height, count, at, device, send, recv):
        def start(*values):
            mine = buffer.at[which, at, pl.ds(0, height)]
            for k, value in enumerate(values):
                buffer[which, at, k * EDGE : (k + 1) * EDGE] = value
            for k in range(1, count):
                pltpu.make_async_remote_copy(
                    src_ref=mine,
                    dst_ref=mine,
                    send_sem=send.at[which],
                    recv_sem=recv.at[which],
                    device_id=device(k),
                    device_id_type=MESH,
                ).start()

        def wait(sem):
            rest = buffer.at[which, pl.ds(0, count - 1), pl.ds(0, height)]
            pltpu.make_async_copy(rest, rest, sem.at[which]).wait()

        def collect():
            wait(recv)
            return tree_sum([buffer[which, k, 0:height] for k in range(count)])

        return start, collect, lambda: wait(send)

    def near_stage(which):
        return stage(near_ref, which, EDGE, near_count, near_at, near_device, near_send, near_recv)

    def far_stage(which):
        return stage(far_ref, which, EDGE, row_count, row_at, far_device, far_send, far_recv)

    def all_stage(which):
        if total <= 32:
            return stage(every, which, EDGE, total, position, any_device, all_send, all_recv)
        first, second = near_stage(which + 1), far_stage(which + 1)

        def start(values):
            first[0](values)
            second[0](first[1]())

        def sent():
            first[2]()
            second[2]()

        return start, second[1], sent

    near_x, far_x = near_stage(0), far_stage(0)
    all_y, all_q, all_z = all_stage(0), all_stage(1), all_stage(2)

    tables()
    hear()
    tell()
    block_wait(ph, block_sem.at[1])
    seg[0] = jnp.zeros((vectors, tile), F32)
    for c in range(chunks):
        split_tiles(c)
        if c == row_tiles // chunk - 1:
            diagonal(xh, yh, reach)
    hear()
    tell()
    halo_start(p_halo)
    diagonal(ph, q_buf, 0)
    x_parts, p_parts = parts(xh, reach), parts(ph, reach)
    near_x[0](pack(inner((x_parts, p_parts), (x_parts, p_parts)), 2 * vectors))

    hear_rest()
    halo_arrived(x_halo)
    scattered(xh, yh, reach)
    halo_start(y_halo)
    y_parts = parts(yh, reach)
    basis = (x_parts, y_parts, p_parts)
    all_y[0](pack(inner(basis, (y_parts,)), vectors))

    far_x[0](near_x[1]())
    halo_arrived(p_halo)
    scattered(ph, q_buf, 0)
    all_q[0](pack(inner(basis, (parts(q_buf, 0),)), vectors))
    diagonal(yh, z_buf, 0)
    halo_arrived(y_halo)
    scattered(yh, z_buf, 0)
    all_z[0](pack(inner(basis, (parts(z_buf, 0),)), vectors))

    scale = 1.0 / vertex_total
    locked = locked_ref[0]
    by_xp = unpack(far_x[1](), 2 * vectors, 2 * vectors)
    by_y = unpack(all_y[1](), width, vectors)
    lane_w = iota((vectors, 128), 1)
    line_w = iota((vectors, 128), 0)
    middle_w = (lane_w >= vectors) & (lane_w < 2 * vectors)
    shifted_y = pltpu.roll(by_y, vectors, 1)
    shifted_xp = pltpu.roll(by_xp, vectors, 1)
    on_first = lane_w == line_w
    on_second = lane_w == line_w + vectors
    free_down = iota((vectors, 1), 0) >= locked
    free_along = (iota((1, 128), 1) >= vectors + locked) & (iota((1, 128), 1) < 2 * vectors)

    def diagonal_of(mask, values, axis):
        return jnp.sum(jnp.where(mask, values, 0.0), axis=axis, keepdims=True)

    def ratio(mask, over, under, axis):
        return (diagonal_of(mask, over, axis) + 1e-06) / (diagonal_of(mask, under, axis) + 1e-06)

    down = jnp.where(free_down, ratio(on_first, by_y[:vectors], by_xp[:vectors], 1), 0.0)
    along = jnp.where(
        free_along, ratio(on_second, shifted_y[:vectors], shifted_xp[:vectors], 0), 0.0
    )

    lane = iota((width, 128), 1)
    line = iota((width, 128), 0)
    is_first = lane < vectors
    is_second = (lane >= vectors) & (lane < 2 * vectors)
    is_third = (lane >= 2 * vectors) & (lane < width)
    square = jnp.concatenate(
        [jnp.where(lane < vectors, by_y, 0.0), jnp.zeros((128 - width, 128), F32)], axis=0
    )
    y_rows = jnp.transpose(square)[:vectors]
    zero_w = jnp.zeros((vectors, 128), F32)
    over_x = jnp.concatenate([by_xp[:vectors], y_rows, by_xp[vectors:]], axis=0)
    over_x_next = jnp.concatenate(
        [shifted_xp[:vectors], pltpu.roll(y_rows, vectors, 1), shifted_xp[vectors:]], axis=0
    )
    over_p = jnp.concatenate([shifted_xp[:vectors], y_rows, shifted_xp[vectors:]], axis=0)
    gate = jnp.where(free_along, 1.0, 0.0)

    def residual_rows(values):
        first, second, third = [values[i * vectors : (i + 1) * vectors] for i in range(3)]
        return jnp.concatenate(
            [first, jnp.where(free_down, down * first - second, 0.0), third], axis=0
        )

    def three(first, second, third):
        return jnp.where(
            is_first, first, jnp.where(is_second, second, jnp.where(is_third, third, 0.0))
        )

    gram = residual_rows(
        three(over_x, over_x_next * along - shifted_y * gate, over_p)
    )
    gram = gram * scale

    rest = gram[vectors : 2 * vectors]
    frozen = on_second & (line_w < locked)
    small = jnp.where(middle_w, rest + jnp.where(frozen, 1.0, 0.0), 0.0)
    small = small + jnp.where(lane_w == line_w + 2 * vectors, 1.0, 0.0)
    padded = (line == lane) & (line >= vectors) & (line < vectors + locked)
    big = gram + jnp.where(padded | (lane == line + width), 1.0, 0.0)

    step = 4
    small_rows = []
    for k in range(0, vectors, step):
        small, done = panel(small, k, vectors, step)
        small_rows += done
    inverse_w = jnp.concatenate(small_rows, axis=0)[:, 2 * vectors : 3 * vectors]

    def outputs():
        high, low = split(inverse_w)
        lhs = jnp.concatenate(
            [jnp.concatenate([high, high], axis=1), jnp.concatenate([low, low], axis=1)], axis=0
        )

        def turn(values):
            rhs = jnp.concatenate(split(values), axis=0)
            out = jnp.dot(lhs, rhs, preferred_element_type=F32)
            return out[:vectors] + out[vectors:]

        for t in range(row_tiles):
            lanes = slice(t * tile, (t + 1) * tile)
            image = yh[reach + t]
            residual = jnp.where(free_down, down * xh[reach + t] - image, 0.0)
            carried = jnp.where(free_down, down * image - z_buf[t], 0.0)
            w_ref[:, lanes] = turn(residual)
            aw_ref[:, lanes] = turn(residual - carried)

    for k in range(0, width, step):
        if k == 2 * vectors:
            outputs()
        big, done = panel(big, k, 0, step)
        for i in range(step):
            upper[k + i : k + i + 1, :] = done[i]
    inverse = upper[:, width : 2 * width]

    by_q = unpack(all_q[1](), width, vectors, 2 * vectors)
    early = residual_rows(three(by_y, shifted_y * along, by_q))
    image = (gram - scale * early)[:, :width]
    half = jnp.dot(inverse, image, precision=HIGHEST, preferred_element_type=F32)
    first = lax.dot_general(half, inverse, NT_DIMS, precision=HIGHEST, preferred_element_type=F32)
    second = lax.dot_general(inverse, half, NT_DIMS, precision=HIGHEST, preferred_element_type=F32)
    base = first + second
    inverse_high, inverse_low = split(inverse)
    left = jnp.concatenate([inverse_high, inverse_low, inverse_high], axis=1)
    right = jnp.concatenate([inverse_high, inverse_high, inverse_low], axis=1)

    by_z = unpack(all_z[1](), width, vectors, vectors)
    late = residual_rows(by_z)[:, :width]
    late = jnp.where(is_second[:, :width], late, 0.0) * gate[:, :width]
    late_high, late_low = split(late * scale)
    half = jnp.dot(
        left,
        jnp.concatenate([late_high, late_high, late_low], axis=0),
        preferred_element_type=F32,
    )
    half_high, half_low = split(half)
    half = jnp.concatenate([half_high, half_low, half_high], axis=1)
    first = lax.dot_general(half, right, NT_DIMS, preferred_element_type=F32)
    second = lax.dot_general(right, half, NT_DIMS, preferred_element_type=F32)
    ritz_ref[...] = 0.5 * (base + (first + second))

    halo_sent(x_halo)
    halo_sent(p_halo)
    halo_sent(y_halo)
    for done in (near_x, far_x, all_y, all_q, all_z):
        done[2]()


def store_kernel(w_ref, aw_ref, ritz_ref, w_hbm, aw_hbm, ritz_hbm, sem):
    copies = [
        pltpu.make_async_copy(source, target, sem.at[i])
        for i, (source, target) in enumerate(
            ((w_ref, w_hbm), (aw_ref, aw_hbm), (ritz_ref, ritz_hbm))
        )
    ]
    for copy in copies:
        copy.start()
    for copy in copies:
        copy.wait()


def body(sizes, current_block, previous_block, adjacency_tiles, tile_rows, tile_cols, tile_count, locked):
    vectors, here = current_block.shape
    slots, tile, _ = adjacency_tiles.shape
    row_tiles = here // tile
    row_count, col_count, sub_count = sizes
    near_count = col_count * sub_count
    total = row_count * near_count
    width = 3 * vectors
    spare = slots - row_tiles
    stages = 1 if total <= 32 else 4
    vmem = pl.BlockSpec(memory_space=pltpu.VMEM)
    anywhere = pl.BlockSpec(memory_space=pl.ANY)
    dma = pltpu.SemaphoreType.DMA
    grid = (2 * row_tiles, vectors, tile)
    own = (row_tiles, vectors, tile)
    shapes = (
        jax.ShapeDtypeStruct((vectors, here), F32),
        jax.ShapeDtypeStruct((vectors, here), F32),
        jax.ShapeDtypeStruct((width, width), F32),
    )
    iterate = pl.pallas_call(
        functools.partial(iterate_kernel, sizes, here * total),
        out_shape=shapes,
        in_specs=[anywhere] * 7,
        out_specs=(vmem, vmem, vmem),
        scratch_shapes=[
            pltpu.SMEM((slots,), jnp.int32),
            pltpu.SMEM((slots,), jnp.int32),
            pltpu.SMEM((1,), jnp.int32),
            pltpu.SMEM((1,), jnp.int32),
            pltpu.SMEM((spare,), jnp.int32),
            pltpu.SMEM((spare,), jnp.int32),
            pltpu.SMEM((row_tiles,), jnp.int32),
            pltpu.VMEM((slots, tile, tile), F32),
            pltpu.VMEM((slots, 2 * tile, tile), BF16),
            pltpu.VMEM(grid, F32),
            pltpu.VMEM(grid, F32),
            pltpu.VMEM(grid, F32),
            pltpu.VMEM(own, F32),
            pltpu.VMEM(own, F32),
            pltpu.VMEM((spare + 1, vectors, tile), F32),
            pltpu.VMEM((stages, near_count, EDGE, 128), F32),
            pltpu.VMEM((stages, row_count, EDGE, 128), F32),
            pltpu.VMEM((3, total, EDGE, 128), F32),
            pltpu.VMEM((width, 128), F32),
            dma((4,)),
            dma((2,)),
            dma((slots // row_tiles,)),
            dma((3, 2)),
            dma((3, 2)),
            dma((stages,)),
            dma((stages,)),
            dma((stages,)),
            dma((stages,)),
            dma((3,)),
            dma((3,)),
            pltpu.SemaphoreType.REGULAR((2,)),
        ],
        compiler_params=pltpu.CompilerParams(
            collective_id=0, has_side_effects=True, vmem_limit_bytes=VMEM_ALL - VMEM_ROOM
        ),
        name="iterate",
    )
    results = lax.cond(
        lax.axis_index("rows") >= 0,
        iterate,
        lambda *_: tuple(jnp.zeros(shape.shape, F32) for shape in shapes),
        tile_cols, tile_rows, tile_count, locked, current_block, previous_block, adjacency_tiles,
    )
    return pl.pallas_call(
        store_kernel,
        out_shape=shapes,
        in_specs=[vmem] * 3,
        out_specs=(anywhere,) * 3,
        scratch_shapes=[dma((3,))],
        compiler_params=pltpu.CompilerParams(vmem_limit_bytes=VMEM_ALL - VMEM_ROOM),
        name="store",
    )(*results)


def solution(mesh):
    split_all = ("graphs", "rows", "cols", "sub")
    sizes = tuple(mesh.shape[name] for name in ("rows", "cols", "sub"))
    in_specs = (
        P(None, split_all),
        P(None, split_all),
        P(split_all, None, None),
        P(split_all),
        P(split_all),
        P(split_all),
        P("graphs"),
    )
    out_specs = (P(None, split_all), P(None, split_all), P("graphs", None))
    return jax.shard_map(
        functools.partial(body, sizes), mesh=mesh, in_specs=in_specs, out_specs=out_specs, check_vma=False
    )
```
